32 devices in a mesh: chain: 16 (over z, x, core), shard: 2 (over y).
Axes of the slice: x: 2, y: 2, z: 4, core: 2. Of those that a mesh axis runs over, the one named last changes fastest.
Arguments:
- w_pair: bfloat16 [16, 2, 256, 4096], P('chain', None, 'shard'), may hold values from -6 to 6
- w_down: bfloat16 [16, 256, 4096], P('chain', 'shard'), may hold values from -6 to 6
- tokens: bfloat16 [16, 512, 4096], P('chain', 'shard'), may hold values from -6 to 6
- cotangent: bfloat16 [16, 512, 4096], P('chain', 'shard'), may hold values from -6 to 6
- seq_ids: int32 [16, 512], P('chain', 'shard'), may hold values from 0 to 7, never falling along the last dimension, each value on 1 to 128 neighbouring positions
- msg_left: bfloat16 [16, 2, 256, 4096], P('chain', None, 'shard'), may hold values from -9 to 9
- msg_right: bfloat16 [16, 2, 256, 4096], P('chain', None, 'shard'), may hold values from -9 to 9
- count_left: int32 [16], P('chain'), may hold values from 0 to 5, as said below
- count_right: int32 [16], P('chain'), may hold values from 0 to 5, as said below
Outputs:
- new_pair: bfloat16 [16, 2, 256, 4096], P('chain', None, 'shard')
The draws below stay inside these ranges and needn't reach their ends.
Inputs may be any that keep to these rules, and one draw needn't show every extreme that they name: count_left of worker w is at most min(w, 5); some worker at least 5 from both ends of the chain has count_left equal to 5. count_right of worker w is at most min(15 - w, 5); the same worker has count_right equal to 5.
All inputs are finite; a program needn't handle non-finite values.
Results may differ from the reference program's by a relative error of at most 0.0053.
Values may be sent and summed in bfloat16 or wider, within the bound.
A program may use at most 128 MiB of HBM per device.

```python
import math
import jax
import jax.numpy as jnp
import numpy as np
from jax import lax

D = 4096
SEQS = 8
H = 256
TOKW = 512
MAXLEN = 128
WORKERS = 16


def forced_worker(key):
    return jax.random.randint(jax.random.fold_in(key, 7), (), 5, WORKERS - 5, dtype=jnp.int32)


def capped_counts(key, salt, limits):
    raw_counts = jax.random.randint(jax.random.fold_in(key, salt), (WORKERS,), 0, 6, dtype=jnp.int32)
    worker_index = jnp.arange(WORKERS, dtype=jnp.int32)
    capped = jnp.minimum(raw_counts, jnp.minimum(limits, 5))
    return jnp.where(worker_index == forced_worker(key), 5, capped).astype(jnp.int32)


def draw_count_left(key, part):
    worker_index = jnp.arange(WORKERS, dtype=jnp.int32)
    return capped_counts(key, 11, worker_index)


def draw_count_right(key, part):
    worker_index = jnp.arange(WORKERS, dtype=jnp.int32)
    return capped_counts(key, 13, WORKERS - 1 - worker_index)


def block_scale(rng, dims, pieces, smallest, top_value):
    def one(position, blocks):
        draws = jax.random.uniform(jax.random.fold_in(jax.random.fold_in(rng, 6), position), (blocks,), jnp.float32, smallest / len(pieces), top_value / len(pieces))
        return jnp.repeat(jnp.exp(draws), dims[position] // blocks).reshape((-1,) + (1,) * (len(dims) - position - 1))

    factor_of = one(*pieces[0])
    for cut in pieces[1:]:
        factor_of = factor_of * one(*cut)
    return factor_of


def length_profile(number_of, total, bound, lean):
    weights = [(1 << 20) // math.isqrt(grade ** lean) + 1 for grade in range(2, number_of + 1)]
    surplus, holding = total - bound - (number_of - 1), [1] * (number_of - 1)
    while surplus > 0:
        free = [i for i in range(number_of - 1) if holding[i] < bound]
        whole, remaining = sum([weights[i] for i in free]), surplus
        for i in free:
            extra = min(bound - holding[i], max(1, remaining * weights[i] // whole), surplus)
            holding[i] = holding[i] + extra
            surplus = surplus - extra
    return np.array([bound] + holding)


def ragged(rng, amount, total, bound, lean):
    if amount == 2:
        one = jax.random.randint(rng, (), max(1, total - bound), min(bound, total - 1) + 1)
        return jnp.stack([one, total - one])
    tallies = jnp.asarray(length_profile(amount, total, bound, lean), jnp.int32)
    couples = (amount - 1) // 2
    source_of, sink = tallies[1:1 + 2 * couples:2], tallies[2:2 + 2 * couples:2]
    margin = jnp.minimum(source_of - 1, bound - sink)
    moved = jax.random.randint(jax.random.fold_in(rng, 1), (couples,), 0, 1 << 20) % (margin + 1)
    tallies = tallies.at[1:1 + 2 * couples:2].set(source_of - moved).at[2:2 + 2 * couples:2].set(sink + moved)
    return tallies[jax.random.permutation(jax.random.fold_in(rng, 2), amount)]


def normal_values(key, dims, width, reach, split=(), kind=jnp.bfloat16):
    entries = jax.random.normal(key, dims, jnp.float32) * width
    if len(split) > 0:
        entries = block_scale(key, dims, split, -0.22, 0.18) * entries
    return jnp.clip(entries, min=-reach, max=reach).astype(kind)


def setup_inputs(seed: int = 0) -> dict:
    key_list = jax.random.split(jax.random.key(seed), 10)
    w_pair = normal_values(key_list[0], (WORKERS, 2, H, D), 1.0, 6.0, ((0, 16), (2, 2)))
    w_down = normal_values(key_list[1], (WORKERS, H, D), 1.0, 6.0, ((0, 16), (1, 2)))
    tokens = normal_values(key_list[2], (WORKERS, TOKW, D), 1.0, 6.0, ((0, 16), (1, 2)))
    cotangent = normal_values(key_list[3], (WORKERS, TOKW, D), 1.0, 6.0, ((0, 16), (1, 2)))
    seq_ids = jax.vmap(lambda own: jnp.searchsorted(jnp.cumsum(ragged(own, SEQS, TOKW, MAXLEN, 1)), jnp.arange(TOKW), side="right"))(jax.random.split(key_list[4], WORKERS)).reshape((WORKERS, TOKW)).astype(jnp.int32)
    msg_left = normal_values(key_list[5], (WORKERS, 2, H, D), 1.5, 9.0, ((0, 16), (2, 2)))
    msg_right = normal_values(key_list[6], (WORKERS, 2, H, D), 1.5, 9.0, ((0, 16), (2, 2)))
    count_left = draw_count_left(jax.random.fold_in(key_list[9], 71), 0)
    count_right = draw_count_right(jax.random.fold_in(key_list[9], 71), 0)
    return {"w_pair": w_pair, "w_down": w_down, "tokens": tokens, "cotangent": cotangent, "seq_ids": seq_ids, "msg_left": msg_left, "msg_right": msg_right, "count_left": count_left, "count_right": count_right}


learn_rate = 1.0


def worker_half(packed):
    w_pair_one, w_down_one, tokens_one, cotangent_one, seq_one = packed
    width_scale = D ** -0.5
    gate_pre = jnp.dot(tokens_one, w_pair_one[0].T, preferred_element_type=jnp.float32) * width_scale
    up_pre = jnp.dot(tokens_one, w_pair_one[1].T, preferred_element_type=jnp.float32) * width_scale
    one_hot = (seq_one[:, None] == jnp.arange(SEQS, dtype=jnp.int32)[None, :]).astype(jnp.float32)
    seq_count = jnp.sum(one_hot, axis=0)
    seq_len = jnp.sum(one_hot * seq_count[None, :], axis=1)
    tok_weight = (TOKW / SEQS) / seq_len
    scaled_cot = (tok_weight[:, None] * cotangent_one.astype(jnp.float32)).astype(jnp.bfloat16)
    grad_hidden = jnp.dot(scaled_cot, w_down_one.T, preferred_element_type=jnp.float32) * width_scale
    sigmoid_gate = jax.nn.sigmoid(gate_pre)
    grad_gate = (grad_hidden * up_pre * sigmoid_gate * (1.0 + gate_pre * (1.0 - sigmoid_gate))).astype(jnp.bfloat16)
    grad_up = (grad_hidden * gate_pre * sigmoid_gate).astype(jnp.bfloat16)
    batch_scale = TOKW ** -0.5
    gate_weight_grad = jnp.dot(grad_gate.T, tokens_one, preferred_element_type=jnp.float32) * batch_scale
    up_weight_grad = jnp.dot(grad_up.T, tokens_one, preferred_element_type=jnp.float32) * batch_scale
    return w_pair_one.astype(jnp.float32) - learn_rate * jnp.stack([gate_weight_grad, up_weight_grad])


def reference(w_pair, w_down, tokens, cotangent, seq_ids, msg_left, msg_right, count_left, count_right):
    half_step = lax.map(worker_half, (w_pair, w_down, tokens, cotangent, seq_ids))
    send_right = (half_step + msg_left.astype(jnp.float32)).astype(jnp.bfloat16)
    send_left = (half_step + msg_right.astype(jnp.float32)).astype(jnp.bfloat16)
    zero_msg = jnp.zeros_like(send_right[:1])
    recv_left = jnp.concatenate([zero_msg, send_right[:-1]], axis=0)
    recv_right = jnp.concatenate([send_left[1:], zero_msg], axis=0)
    zero_count = jnp.zeros((1,), jnp.int32)
    cnt_left = jnp.concatenate([zero_count, (count_left[:-1] + 1).astype(jnp.int32)], axis=0)
    cnt_right = jnp.concatenate([(count_right[1:] + 1).astype(jnp.int32), zero_count], axis=0)
    total_count = (1 + cnt_left + cnt_right).astype(jnp.float32)
    summed = half_step + recv_left.astype(jnp.float32) + recv_right.astype(jnp.float32)
    return (summed / total_count[:, None, None, None]).astype(jnp.bfloat16)
```

```python
import functools

import jax
import jax.numpy as jnp
from jax import lax
from jax.experimental import pallas as pl
from jax.experimental.pallas import tpu as pltpu
from jax.sharding import PartitionSpec as P

SEQS = 8
learn_rate = 1.0

MESH = pl.DeviceIdType.MESH
F32 = jnp.float32
BF16 = jnp.bfloat16

BLOCKS = 8
CHUNKS = 8
GROUPS = 4
PER = CHUNKS // GROUPS
ODD_PLAN = (2, 0, 2, 0, 4)
EVEN_PLAN = (4, 1, 1, 2, 0)
AHEAD = 2


def reach(plan):
    total, out = 0, []
    for count in plan:
        total += count
        out.append(total)
    return out


ODD_REACH, EVEN_REACH = reach(ODD_PLAN), reach(EVEN_PLAN)


def stage_of(ends, j):
    return next(i for i, end in enumerate(ends) if j < end)


def dot_last(a, b):
    return lax.dot_general(a, b, (((1,), (1,)), ((), ())), preferred_element_type=F32)


def dot_plain(a, b):
    return lax.dot_general(a, b, (((1,), (0,)), ((), ())), preferred_element_type=F32)


def kernel(
    n,
    w_hbm, wd_hbm, tok_hbm, cot_hbm, ml_hbm, mr_hbm, ids_hbm, cl_hbm, cr_hbm,
    out_v,
    w_v, wd_v, tok_v, cot_v, mm_v, mx_v, ids_v, cl_s, cr_s,
    wdp_v, tokp_v, ids_p, gh_s, gh_r,
    acc, acc_r, s_m, s_x, r_m, r_x, tf, g_s, g_x, c_m, c_x, k_m, k_x,
    st_wd, st_tok,
    load_sem, ids_sem, wd_sem, gh_sem, tok_ss, tok_rs,
    msgm_sem, msgx_sem, fwd_sem, g_sem, cnt_sem, stage_sem, mate_ss,
):
    c = lax.axis_index("chain")
    s = lax.axis_index("shard")
    odd = lax.rem(c, 2) == 1
    even = lax.rem(c, 2) == 0
    sign = 2 * lax.rem(c, 2) - 1
    mate_c, cross_c = c - sign, c + sign
    has_cross = jnp.logical_and(cross_c >= 0, cross_c < n)
    mate, cross, peer, across = (mate_c, s), (cross_c, s), (c, 1 - s), (mate_c, 1 - s)
    tokens, depth = tok_v.shape
    hidden = wd_v.shape[0]
    block = depth // BLOCKS
    chunk = tokens // CHUNKS
    group = tokens // GROUPS
    width_scale = depth ** (-0.5)
    batch_scale = learn_rate * (2 * tokens) ** (-0.5)

    def local(src, dst, i):
        return pltpu.make_async_copy(src, dst, load_sem.at[i])

    loads = [
        local(src, dst, i)
        for i, (src, dst) in enumerate(
            [(ids_hbm, ids_v), (tok_hbm, tok_v), (w_hbm, w_v), (wd_hbm, wd_v), (cot_hbm, cot_v)]
        )
    ]
    count_loads = [local(cl_hbm, cl_s, 7), local(cr_hbm, cr_s, 8)]
    for load in loads + count_loads:
        load.start()

    barrier = pltpu.get_barrier_semaphore()
    for where in (peer, across, mate):
        pl.semaphore_signal(barrier, inc=1, device_id=where, device_id_type=MESH)

    @pl.when(has_cross)
    def _():
        pl.semaphore_signal(barrier, inc=1, device_id=cross, device_id_type=MESH)

    msg_even = [local(ml_hbm, mm_v, 5), local(mr_hbm, mx_v, 6)]
    msg_odd = [local(mr_hbm, mm_v, 5), local(ml_hbm, mx_v, 6)]

    @pl.when(even)
    def _():
        for load in msg_even:
            load.start()

    @pl.when(odd)
    def _():
        for load in msg_odd:
            load.start()

    def remote(src, dst, send_sem, recv_sem, where):
        return pltpu.make_async_remote_copy(
            src_ref=src, dst_ref=dst, send_sem=send_sem, recv_sem=recv_sem, device_id=where, device_id_type=MESH
        )

    def cols(j):
        return slice(j * block, (j + 1) * block)

    def rows(k):
        return slice(k * chunk, (k + 1) * chunk)

    def span(q):
        return slice(q * group, (q + 1) * group)

    ids_copy = remote(ids_hbm, ids_p, ids_sem.at[0], ids_sem.at[1], peer)
    wd_copy = remote(wd_hbm, wdp_v, wd_sem.at[0], wd_sem.at[1], peer)
    gh_copy = remote(gh_s, gh_r, gh_sem.at[0], gh_sem.at[1], peer)
    tok_copy = [
        remote(tok_hbm.at[rows(k)], tokp_v.at[rows(k)], tok_ss.at[k], tok_rs.at[k], peer) for k in range(CHUNKS)
    ]
    half_tok = tokens // 2
    stage_copy = [remote(wd_hbm, st_wd, stage_sem.at[0, 0], stage_sem.at[1, 0], mate)] + [
        remote(
            tok_hbm.at[i * half_tok : (i + 1) * half_tok],
            st_tok.at[i * half_tok : (i + 1) * half_tok],
            stage_sem.at[0, i + 1],
            stage_sem.at[1, i + 1],
            mate,
        )
        for i in range(2)
    ]
    mate_copy = [remote(st_wd, wdp_v, mate_ss.at[0], wd_sem.at[1], across)] + [
        remote(st_tok.at[rows(k)], tokp_v.at[rows(k)], mate_ss.at[k + 1], tok_rs.at[k], across) for k in range(CHUNKS)
    ]
    msgm_copy = [remote(s_m.at[j], r_m.at[j], msgm_sem.at[0, j], msgm_sem.at[1, j], mate) for j in range(BLOCKS)]
    msgx_copy = [remote(s_x.at[j], r_x.at[j], msgx_sem.at[0, j], msgx_sem.at[1, j], cross) for j in range(BLOCKS)]

    def fwd_copy(ends, k):
        wide = ends[k // PER] * block
        return remote(tokp_v.at[rows(k), :wide], tf.at[rows(k), :wide], fwd_sem.at[0, k], fwd_sem.at[1, k], cross)

    g_copy = [remote(g_s.at[q], g_x.at[q], g_sem.at[0, q], g_sem.at[1, q], cross) for q in range(GROUPS)]
    cnt_m = remote(c_m, k_m, cnt_sem.at[0, 0], cnt_sem.at[1, 0], mate)
    cnt_x = remote(c_x, k_x, cnt_sem.at[0, 1], cnt_sem.at[1, 1], cross)

    odd_cross = jnp.logical_and(odd, has_cross)
    even_cross = jnp.logical_and(even, has_cross)
    plans = ((odd_cross, ODD_REACH), (even_cross, EVEN_REACH))

    @pl.when(jnp.logical_not(has_cross))
    def _():
        for ref in (r_x, tf, g_x, k_x):
            ref[...] = jnp.zeros_like(ref)

    pl.semaphore_wait(barrier, 3 + has_cross.astype(jnp.int32))
    ids_copy.start()

    @pl.when(even)
    def _():
        for copy in stage_copy:
            copy.start()

    @pl.when(odd)
    def _():
        wd_copy.start()
        for k in range(AHEAD):
            tok_copy[k].start()

    def gates(pre, grad_hidden):
        gate_pre, up_pre = pre[:hidden] * width_scale, pre[hidden:] * width_scale
        sig = jax.nn.sigmoid(gate_pre)
        grad_gate = grad_hidden * up_pre * sig * (1.0 + gate_pre * (1.0 - sig))
        grad_up = grad_hidden * gate_pre * sig
        return jnp.concatenate([grad_gate, grad_up], axis=0)

    def send_cross(j):
        s_x[j] = (acc[:, cols(j)] + mx_v[:, cols(j)].astype(F32)).astype(BF16)
        msgx_copy[j].start()

    def send_stage(stage, j):
        for active, ends in plans:
            if stage_of(ends, j) == stage:

                @pl.when(active)
                def _():
                    send_cross(j)

    for load in loads[1:3]:
        load.wait()
    pre_own = dot_last(w_v[...], tok_v[...])
    for load in loads[3:] + loads[:1]:
        load.wait()
    down_own = dot_last(wd_v[...], cot_v[...])
    one_hot = (lax.broadcasted_iota(jnp.int32, (SEQS, tokens), 0) == ids_v[...]).astype(F32)
    ids_copy.wait_recv()
    other_hot = (lax.broadcasted_iota(jnp.int32, (SEQS, tokens), 0) == ids_p[...]).astype(F32)
    total = jnp.sum(one_hot + other_hot, axis=1, keepdims=True)
    seq_len = jnp.sum(one_hot * total, axis=0, keepdims=True)
    tok_weight = (2 * tokens / SEQS) / seq_len * width_scale
    g_own = gates(pre_own, down_own * tok_weight).astype(BF16)
    for load in msg_even:
        load.wait()
    for j in range(BLOCKS):
        acc[:, cols(j)] = w_v[:, cols(j)].astype(F32) - dot_plain(g_own, tok_v[:, cols(j)]) * batch_scale
        send_stage(0, j)

    for load in count_loads:
        load.wait()
    c_m[...] = jnp.full(c_m.shape, 1 + jnp.where(odd, cr_s[0], cl_s[0]), jnp.int32).astype(F32)
    c_x[...] = jnp.full(c_x.shape, 1 + jnp.where(odd, cl_s[0], cr_s[0]), jnp.int32).astype(F32)
    cnt_m.start()

    @pl.when(has_cross)
    def _():
        cnt_x.start()

    wd_copy.wait_recv()
    gh_s[...] = (dot_last(wdp_v[...], cot_v[...]) * tok_weight).astype(BF16)
    gh_copy.start()

    @pl.when(odd)
    def _():
        for k in range(AHEAD, CHUNKS):
            tok_copy[k].start()
        for copy in stage_copy:
            copy.wait_recv()
        for copy in mate_copy:
            copy.start()

    cnt_m.wait_recv()

    @pl.when(has_cross)
    def _():
        cnt_x.wait_recv()

    inverse = 1.0 / (1.0 + k_m[0:1, 0:1] + k_x[0:1, 0:1])

    def cross_grad(q):
        return g_x[q].astype(F32).T.astype(BF16)

    def wait_cross(copies):
        @pl.when(has_cross)
        def _():
            for copy in copies:
                copy.wait_recv()

    def wait_forward(ends, q):
        wait_cross(
            [fwd_copy(ends, k) for k in range(q * PER, (q + 1) * PER) if ends[q] > 0] + ([g_copy[q]] if ends[q] > 0 else [])
        )

    def own(q):
        for k in range(q * PER, (q + 1) * PER):
            tok_copy[k].wait_recv()
            for active, ends in plans:
                if ends[q] > 0:

                    @pl.when(active)
                    def _():
                        fwd_copy(ends, k).start()

        pre = dot_last(w_v[...], tokp_v[span(q)])
        if q == 0:
            gh_copy.wait_recv()
        g_now = gates(pre, gh_r[:, span(q)].astype(F32))
        g_s[q] = g_now.T.astype(BF16)
        for active, ends in plans:
            if ends[q] > 0:

                @pl.when(active)
                def _():
                    g_copy[q].start()

        g_now = g_now.astype(BF16)
        first = [j for j in range(BLOCKS) if any(stage_of(ends, j) == q + 1 for _, ends in plans)]
        for j in first + [j for j in range(BLOCKS) if j not in first]:
            acc[:, cols(j)] = acc[:, cols(j)] - dot_plain(g_now, tokp_v[span(q), cols(j)]) * batch_scale
            send_stage(q + 1, j)
            if q == GROUPS - 1:
                s_m[j] = (acc[:, cols(j)] + mm_v[:, cols(j)].astype(F32)).astype(BF16)
                msgm_copy[j].start()

    def correction(q, j):
        return dot_plain(cross_grad(q), tf[span(q), cols(j)]) * batch_scale

    def gather_even():
        for q in range(GROUPS):
            wait_forward(ODD_REACH, q)
        grads = {}
        for j in range(BLOCKS):
            msgm_copy[j].wait_recv()
            wait_cross([msgx_copy[j]])
            value = r_m[j].astype(F32) + r_x[j].astype(F32)
            start = stage_of(ODD_REACH, j)
            if start < GROUPS:
                if start not in grads:
                    grads[start] = jnp.concatenate([cross_grad(q) for q in range(start, GROUPS)], axis=1)
                value = value - dot_plain(grads[start], tf[start * group :, cols(j)]) * batch_scale
            acc_r[:, cols(j)] = value

    def gather_odd():
        for q in range(GROUPS):
            wait_forward(EVEN_REACH, q)
            g_now = cross_grad(q)
            for j in range(BLOCKS):
                start = stage_of(EVEN_REACH, j)
                if start > q and q < GROUPS - 1:
                    continue
                value = acc[:, cols(j)]
                if start <= q:
                    value = value - dot_plain(g_now, tf[span(q), cols(j)]) * batch_scale
                if start == q or (q == GROUPS - 1 and start == GROUPS):
                    wait_cross([msgx_copy[j]])
                    value = value + r_x[j].astype(F32)
                if q < GROUPS - 1:
                    acc[:, cols(j)] = value
                else:
                    msgm_copy[j].wait_recv()
                    out_v[:, cols(j)] = ((value + r_m[j].astype(F32)) * inverse).astype(BF16)

    own(0)
    own(1)

    @pl.when(even)
    def _():
        gather_even()

    own(2)
    own(3)

    @pl.when(even)
    def _():
        for j in range(BLOCKS):
            out_v[:, cols(j)] = ((acc[:, cols(j)] + acc_r[:, cols(j)]) * inverse).astype(BF16)

    @pl.when(odd)
    def _():
        gather_odd()

    for copy in [ids_copy, gh_copy, cnt_m] + msgm_copy:
        copy.wait_send()

    @pl.when(even)
    def _():
        for copy in stage_copy:
            copy.wait_send()

    @pl.when(odd)
    def _():
        for copy in [wd_copy] + tok_copy + mate_copy:
            copy.wait_send()

    @pl.when(has_cross)
    def _():
        for copy in msgx_copy + [cnt_x]:
            copy.wait_send()

    for active, ends in plans:

        @pl.when(active)
        def _():
            for q in range(GROUPS):
                if ends[q] > 0:
                    g_copy[q].wait_send()
                    for k in range(q * PER, (q + 1) * PER):
                        fwd_copy(ends, k).wait_send()


def body(n, w_pair, w_down, tokens, cotangent, seq_ids, msg_left, msg_right, count_left, count_right):
    _, two, hidden, depth = w_pair.shape
    rows = tokens.shape[1]
    flat = (two * hidden, depth)
    block = depth // BLOCKS
    hbm = pl.BlockSpec(memory_space=pltpu.HBM)
    dma = pltpu.SemaphoreType.DMA
    blocked = (BLOCKS, two * hidden, block)
    grads = (GROUPS, rows // GROUPS, two * hidden)
    vmem = pltpu.VMEM
    out = pl.pallas_call(
        functools.partial(kernel, n),
        out_shape=vmem(flat, BF16),
        in_specs=[hbm] * 9,
        out_specs=pl.BlockSpec(memory_space=vmem),
        scratch_shapes=[
            vmem(flat, BF16),
            vmem((hidden, depth), BF16),
            vmem((rows, depth), BF16),
            vmem((rows, depth), BF16),
            vmem(flat, BF16),
            vmem(flat, BF16),
            vmem((1, rows), jnp.int32),
            pltpu.SMEM((1,), jnp.int32),
            pltpu.SMEM((1,), jnp.int32),
            vmem((hidden, depth), BF16),
            vmem((rows, depth), BF16),
            vmem((1, rows), jnp.int32),
            vmem((hidden, rows), BF16),
            vmem((hidden, rows), BF16),
            vmem(flat, F32),
            vmem(flat, F32),
            vmem(blocked, BF16),
            vmem(blocked, BF16),
            vmem(blocked, BF16),
            vmem(blocked, BF16),
            vmem((rows, depth), BF16),
            vmem(grads, BF16),
            vmem(grads, BF16),
            vmem((8, 128), F32),
            vmem((8, 128), F32),
            vmem((8, 128), F32),
            vmem((8, 128), F32),
            vmem((hidden, depth), BF16),
            vmem((rows, depth), BF16),
            dma((9,)),
            dma((2,)),
            dma((2,)),
            dma((2,)),
            dma((CHUNKS,)),
            dma((CHUNKS,)),
            dma((2, BLOCKS)),
            dma((2, BLOCKS)),
            dma((2, CHUNKS)),
            dma((2, GROUPS)),
            dma((2, 2)),
            dma((2, 3)),
            dma((CHUNKS + 1,)),
        ],
        compiler_params=pltpu.CompilerParams(
            collective_id=0, has_side_effects=True, vmem_limit_bytes=60 * 1024 * 1024
        ),
    )(
        w_pair.reshape(flat),
        w_down[0],
        tokens[0],
        cotangent[0],
        msg_left.reshape(flat),
        msg_right.reshape(flat),
        seq_ids,
        count_left,
        count_right,
    )
    return out.reshape(w_pair.shape)


def solution(mesh):
    return jax.shard_map(
        functools.partial(body, mesh.shape["chain"]),
        mesh=mesh,
        in_specs=(
            P("chain", None, "shard", None),
            P("chain", "shard", None),
            P("chain", "shard", None),
            P("chain", "shard", None),
            P("chain", "shard"),
            P("chain", None, "shard", None),
            P("chain", None, "shard", None),
            P("chain"),
            P("chain"),
        ),
        out_specs=P("chain", None, "shard", None),
        check_vma=False,
    )
```

```python
import functools

import jax
import jax.numpy as jnp
from jax import lax
from jax.experimental import pallas as pl
from jax.experimental.pallas import tpu as pltpu
from jax.sharding import PartitionSpec as P

SEQS = 8
learn_rate = 1.0

MESH = pl.DeviceIdType.MESH
F32 = jnp.float32
BF16 = jnp.bfloat16

BLOCKS = 8
CHUNKS = 8
GROUPS = 4
PER = CHUNKS // GROUPS
ODD_PLAN = (0, 1, 1, 1, 5)
EVEN_PLAN = (7, 0, 0, 0, 1)
AHEAD = 2


def reach(plan):
    total, out = 0, []
    for count in plan:
        total += count
        out.append(total)
    return out


ODD_REACH, EVEN_REACH = reach(ODD_PLAN), reach(EVEN_PLAN)


def stage_of(ends, j):
    return next(i for i, end in enumerate(ends) if j < end)


def dot_last(a, b):
    return lax.dot_general(a, b, (((1,), (1,)), ((), ())), preferred_element_type=F32)


def dot_plain(a, b):
    return lax.dot_general(a, b, (((1,), (0,)), ((), ())), preferred_element_type=F32)


def kernel(
    n,
    w_hbm, wd_hbm, tok_hbm, cot_hbm, ml_hbm, mr_hbm, ids_hbm, cl_hbm, cr_hbm,
    out_v,
    w_v, wd_v, tok_v, cot_v, mm_v, mx_v, ids_v, cl_s, cr_s,
    wdp_v, tokp_v, ids_p, gh_s, gh_r,
    acc, acc_r, s_m, s_x, r_m, r_x, tf, g_s, g_x, c_m, c_x, k_m, k_x,
    st_wd, st_tok, g_keep,
    load_sem, ids_sem, wd_sem, gh_sem, tok_ss, tok_rs,
    msgm_sem, msgx_sem, fwd_sem, g_sem, cnt_sem, stage_sem, mate_ss,
):
    c = lax.axis_index("chain")
    s = lax.axis_index("shard")
    odd = lax.rem(c, 2) == 1
    even = lax.rem(c, 2) == 0
    sign = 2 * lax.rem(c, 2) - 1
    mate_c, cross_c = c - sign, c + sign
    has_cross = jnp.logical_and(cross_c >= 0, cross_c < n)
    mate, cross, peer, across = (mate_c, s), (cross_c, s), (c, 1 - s), (mate_c, 1 - s)
    tokens, depth = tok_v.shape
    hidden = wd_v.shape[0]
    block = depth // BLOCKS
    chunk = tokens // CHUNKS
    group = tokens // GROUPS
    width_scale = depth ** (-0.5)
    batch_scale = learn_rate * (2 * tokens) ** (-0.5)

    def local(src, dst, i):
        return pltpu.make_async_copy(src, dst, load_sem.at[i])

    loads = [
        local(src, dst, i)
        for i, (src, dst) in enumerate(
            [(ids_hbm, ids_v), (tok_hbm, tok_v), (w_hbm, w_v), (wd_hbm, wd_v), (cot_hbm, cot_v)]
        )
    ]
    count_loads = [local(cl_hbm, cl_s, 7), local(cr_hbm, cr_s, 8)]
    for load in loads + count_loads:
        load.start()

    barrier = pltpu.get_barrier_semaphore()
    for where in (peer, across, mate):
        pl.semaphore_signal(barrier, inc=1, device_id=where, device_id_type=MESH)

    @pl.when(has_cross)
    def _():
        pl.semaphore_signal(barrier, inc=1, device_id=cross, device_id_type=MESH)

    msg_even = [local(ml_hbm, mm_v, 5), local(mr_hbm, mx_v, 6)]
    msg_odd = [local(mr_hbm, mm_v, 5), local(ml_hbm, mx_v, 6)]

    @pl.when(even)
    def _():
        for load in msg_even:
            load.start()

    @pl.when(odd)
    def _():
        for load in msg_odd:
            load.start()

    def remote(src, dst, send_sem, recv_sem, where):
        return pltpu.make_async_remote_copy(
            src_ref=src, dst_ref=dst, send_sem=send_sem, recv_sem=recv_sem, device_id=where, device_id_type=MESH
        )

    def cols(j):
        return slice(j * block, (j + 1) * block)

    def rows(k):
        return slice(k * chunk, (k + 1) * chunk)

    def span(q):
        return slice(q * group, (q + 1) * group)

    ids_copy = remote(ids_v, ids_p, ids_sem.at[0], ids_sem.at[1], peer)
    wd_copy = remote(wd_hbm, wdp_v, wd_sem.at[0], wd_sem.at[1], peer)
    gh_copy = remote(gh_s, gh_r, gh_sem.at[0], gh_sem.at[1], peer)
    tok_copy = [
        remote(tok_hbm.at[rows(k)], tokp_v.at[rows(k)], tok_ss.at[k], tok_rs.at[k], peer) for k in range(CHUNKS)
    ]
    half_tok = tokens // 2
    stage_copy = [remote(wd_hbm, st_wd, stage_sem.at[0, 0], stage_sem.at[1, 0], mate)] + [
        remote(
            tok_hbm.at[i * half_tok : (i + 1) * half_tok],
            st_tok.at[i * half_tok : (i + 1) * half_tok],
            stage_sem.at[0, i + 1],
            stage_sem.at[1, i + 1],
            mate,
        )
        for i in range(2)
    ]
    mate_copy = [remote(st_wd, wdp_v, mate_ss.at[0], wd_sem.at[1], across)] + [
        remote(st_tok.at[rows(k)], tokp_v.at[rows(k)], mate_ss.at[k + 1], tok_rs.at[k], across) for k in range(CHUNKS)
    ]
    msgm_copy = [remote(s_m.at[j], r_m.at[j], msgm_sem.at[0, j], msgm_sem.at[1, j], mate) for j in range(BLOCKS)]
    msgx_copy = [remote(s_x.at[j], r_x.at[j], msgx_sem.at[0, j], msgx_sem.at[1, j], cross) for j in range(BLOCKS)]

    def fwd_copy(ends, k):
        wide = ends[k // PER] * block
        return remote(tokp_v.at[rows(k), :wide], tf.at[rows(k), :wide], fwd_sem.at[0, k], fwd_sem.at[1, k], cross)

    g_copy = [remote(g_s.at[q], g_x.at[q], g_sem.at[0, q], g_sem.at[1, q], cross) for q in range(GROUPS)]
    cnt_m = remote(c_m, k_m, cnt_sem.at[0, 0], cnt_sem.at[1, 0], mate)
    cnt_x = remote(c_x, k_x, cnt_sem.at[0, 1], cnt_sem.at[1, 1], cross)

    odd_cross = jnp.logical_and(odd, has_cross)
    even_cross = jnp.logical_and(even, has_cross)
    plans = ((odd_cross, ODD_REACH), (even_cross, EVEN_REACH))

    @pl.when(jnp.logical_not(has_cross))
    def _():
        for ref in (r_x, tf, g_x, k_x):
            ref[...] = jnp.zeros_like(ref)

    loads[0].wait()
    for load in count_loads:
        load.wait()
    c_m[...] = jnp.full(c_m.shape, 1 + jnp.where(odd, cr_s[0], cl_s[0]), jnp.int32).astype(F32)
    c_x[...] = jnp.full(c_x.shape, 1 + jnp.where(odd, cl_s[0], cr_s[0]), jnp.int32).astype(F32)

    with jax.named_scope("barrier"):
        pl.semaphore_wait(barrier, 3 + has_cross.astype(jnp.int32))

    ids_copy.start()

    @pl.when(odd)
    def _():
        wd_copy.start()
        for k in range(AHEAD):
            tok_copy[k].start()

    cnt_m.start()

    @pl.when(has_cross)
    def _():
        cnt_x.start()

    @pl.when(even)
    def _():
        for copy in stage_copy:
            copy.start()

    def gates(pre, grad_hidden):
        gate_pre, up_pre = pre[:hidden] * width_scale, pre[hidden:] * width_scale
        sig = jax.nn.sigmoid(gate_pre)
        grad_gate = grad_hidden * up_pre * sig * (1.0 + gate_pre * (1.0 - sig))
        grad_up = grad_hidden * gate_pre * sig
        return jnp.concatenate([grad_gate, grad_up], axis=0)

    def send_cross(j):
        s_x[j] = (acc[:, cols(j)] + mx_v[:, cols(j)].astype(F32)).astype(BF16)
        msgx_copy[j].start()

    def send_stage(stage, j):
        for active, ends in plans:
            if stage_of(ends, j) == stage:

                @pl.when(active)
                def _():
                    send_cross(j)

    def pre_of(rows_v):
        return dot_last(w_v[...], rows_v)

    with jax.named_scope("load"):
        for load in loads[1:3]:
            load.wait()
    pre_own = pre_of(tok_v[...])
    for load in loads[3:]:
        load.wait()
    down_own = dot_last(wd_v[...], cot_v[...])
    one_hot = (lax.broadcasted_iota(jnp.int32, (SEQS, tokens), 0) == ids_v[...]).astype(F32)
    with jax.named_scope("ids"):
        ids_copy.wait_recv()
    other_hot = (lax.broadcasted_iota(jnp.int32, (SEQS, tokens), 0) == ids_p[...]).astype(F32)
    total = jnp.sum(one_hot + other_hot, axis=1, keepdims=True)
    seq_len = jnp.sum(one_hot * total, axis=0, keepdims=True)
    tok_weight = (2 * tokens / SEQS) / seq_len * width_scale
    g_own = gates(pre_own, down_own * tok_weight).astype(BF16)
    for load in msg_even:
        load.wait()
    for j in range(BLOCKS):
        with jax.named_scope(f"half_{j}"):
            acc[:, cols(j)] = w_v[:, cols(j)].astype(F32) - dot_plain(g_own, tok_v[:, cols(j)]) * batch_scale
            send_stage(0, j)

    with jax.named_scope("wd_wait"):
        wd_copy.wait_recv()
    gh_s[...] = (dot_last(wdp_v[...], cot_v[...]) * tok_weight).astype(BF16)
    gh_copy.start()

    @pl.when(odd)
    def _():
        for k in range(AHEAD, CHUNKS):
            tok_copy[k].start()
        for copy in stage_copy:
            copy.wait_recv()
        for copy in mate_copy:
            copy.start()

    cnt_m.wait_recv()

    @pl.when(has_cross)
    def _():
        cnt_x.wait_recv()

    inverse = 1.0 / (1.0 + k_m[0:1, 0:1] + k_x[0:1, 0:1])

    def cross_grad(q):
        return g_x[q].astype(F32).T.astype(BF16)

    def wait_cross(copies):
        @pl.when(has_cross)
        def _():
            for copy in copies:
                copy.wait_recv()

    def wait_forward(ends, q):
        wait_cross(
            [fwd_copy(ends, k) for k in range(q * PER, (q + 1) * PER) if ends[q] > 0] + ([g_copy[q]] if ends[q] > 0 else [])
        )

    def own(q):
        for k in range(q * PER, (q + 1) * PER):
            with jax.named_scope(f"tok_{k}"):
                tok_copy[k].wait_recv()
            for active, ends in plans:
                if ends[q] > 0:

                    @pl.when(active)
                    def _():
                        fwd_copy(ends, k).start()

        pre = pre_of(tokp_v[span(q)])
        if q == 0:
            with jax.named_scope("gh_wait"):
                gh_copy.wait_recv()
        g_now = gates(pre, gh_r[:, span(q)].astype(F32))
        g_s[q] = g_now.T.astype(BF16)
        for active, ends in plans:
            if ends[q] > 0:

                @pl.when(active)
                def _():
                    g_copy[q].start()

        return g_now.astype(BF16)

    def part(q, j, g_now):
        return acc[:, cols(j)] - dot_plain(g_now, tokp_v[span(q), cols(j)]) * batch_scale

    def own_and_update(q):
        g_now = own(q)
        first = [j for j in range(BLOCKS) if any(stage_of(ends, j) == q + 1 for _, ends in plans)]
        for some in (first, [j for j in range(BLOCKS) if j not in first]):
            for j in some:
                acc[:, cols(j)] = part(q, j, g_now)
            for j in some:
                send_stage(q + 1, j)

    def last_order(ends):
        return sorted(range(BLOCKS), key=lambda j: stage_of(ends, j) < GROUPS)

    def send_last(ends, active, j, value):
        if stage_of(ends, j) == GROUPS:
            s_x[j] = (value + mx_v[:, cols(j)].astype(F32)).astype(BF16)

            @pl.when(active)
            def _():
                msgx_copy[j].start()

    def send_mate(j, value):
        s_m[j] = (value + mm_v[:, cols(j)].astype(F32)).astype(BF16)
        msgm_copy[j].start()

    def finish_even(g_now):
        for j in last_order(EVEN_REACH):
            value = part(GROUPS - 1, j, g_now)
            send_last(EVEN_REACH, even_cross, j, value)
            send_mate(j, value)
            out_v[:, cols(j)] = ((value + acc_r[:, cols(j)]) * inverse).astype(BF16)

    def finish_odd(g_now):
        for j in last_order(ODD_REACH):
            value = part(GROUPS - 1, j, g_now)
            acc[:, cols(j)] = value
            send_last(ODD_REACH, odd_cross, j, value)
        for j in range(BLOCKS):
            send_mate(j, acc[:, cols(j)])

    def gather_even():
        with jax.named_scope("fwd_all"):
            for q in range(GROUPS):
                wait_forward(ODD_REACH, q)
        with jax.named_scope("msgm_all"):
            for copy in msgm_copy:
                copy.wait_recv()
        with jax.named_scope("msgx_all"):
            wait_cross(msgx_copy)
        grads = [cross_grad(q) if ODD_REACH[q] > 0 else None for q in range(GROUPS)]
        for j in range(BLOCKS):
            value = r_m[j].astype(F32) + r_x[j].astype(F32)
            start = stage_of(ODD_REACH, j)
            if start < GROUPS:
                grad = jnp.concatenate(grads[start:], axis=1)
                value = value - dot_plain(grad, tf[start * group :, cols(j)]) * batch_scale
            acc_r[:, cols(j)] = value

    def gather_odd():
        starts = [stage_of(EVEN_REACH, j) for j in range(BLOCKS)]
        for q in range(GROUPS):
            if q == GROUPS - 1:
                with jax.named_scope("msgm_all"):
                    for copy in msgm_copy:
                        copy.wait_recv()
                for j in range(BLOCKS):
                    acc[:, cols(j)] = acc[:, cols(j)] + r_m[j].astype(F32)
            with jax.named_scope(f"fwd_{q}"):
                wait_forward(EVEN_REACH, q)
                wait_cross([msgx_copy[j] for j in range(BLOCKS) if starts[j] == q])
            g_now = cross_grad(q) if EVEN_REACH[q] > 0 else None
            for j in range(BLOCKS):
                if starts[j] > q:
                    continue
                value = acc[:, cols(j)] - dot_plain(g_now, tf[span(q), cols(j)]) * batch_scale
                if starts[j] == q:
                    value = value + r_x[j].astype(F32)
                if q < GROUPS - 1:
                    acc[:, cols(j)] = value
                else:
                    out_v[:, cols(j)] = (value * inverse).astype(BF16)
        for j in range(BLOCKS):
            if starts[j] == GROUPS:
                with jax.named_scope(f"msgx_{j}"):
                    wait_cross([msgx_copy[j]])
                out_v[:, cols(j)] = ((acc[:, cols(j)] + r_x[j].astype(F32)) * inverse).astype(BF16)

    own_and_update(0)
    own_and_update(1)

    @pl.when(even)
    def _():
        gather_even()

    own_and_update(2)
    g_last = own(GROUPS - 1)
    g_keep[...] = g_last

    @pl.when(even)
    def _():
        finish_even(g_keep[...])

    @pl.when(odd)
    def _():
        finish_odd(g_keep[...])
        gather_odd()

    with jax.named_scope("sent"):
        for copy in [ids_copy, gh_copy, cnt_m] + msgm_copy:
            copy.wait_send()

    @pl.when(even)
    def _():
        for copy in stage_copy:
            copy.wait_send()

    @pl.when(odd)
    def _():
        for copy in [wd_copy] + tok_copy + mate_copy:
            copy.wait_send()

    @pl.when(has_cross)
    def _():
        for copy in msgx_copy + [cnt_x]:
            copy.wait_send()

    for active, ends in plans:

        @pl.when(active)
        def _():
            for q in range(GROUPS):
                if ends[q] > 0:
                    g_copy[q].wait_send()
                    for k in range(q * PER, (q + 1) * PER):
                        fwd_copy(ends, k).wait_send()


def body(n, w_pair, w_down, tokens, cotangent, seq_ids, msg_left, msg_right, count_left, count_right):
    _, two, hidden, depth = w_pair.shape
    rows = tokens.shape[1]
    flat = (two * hidden, depth)
    block = depth // BLOCKS
    hbm = pl.BlockSpec(memory_space=pltpu.HBM)
    dma = pltpu.SemaphoreType.DMA
    blocked = (BLOCKS, two * hidden, block)
    grads = (GROUPS, rows // GROUPS, two * hidden)
    vmem = pltpu.VMEM
    out = pl.pallas_call(
        functools.partial(kernel, n),
        out_shape=vmem(flat, BF16),
        in_specs=[hbm] * 9,
        out_specs=pl.BlockSpec(memory_space=vmem),
        scratch_shapes=[
            vmem(flat, BF16),
            vmem((hidden, depth), BF16),
            vmem((rows, depth), BF16),
            vmem((rows, depth), BF16),
            vmem(flat, BF16),
            vmem(flat, BF16),
            vmem((1, rows), jnp.int32),
            pltpu.SMEM((1,), jnp.int32),
            pltpu.SMEM((1,), jnp.int32),
            vmem((hidden, depth), BF16),
            vmem((rows, depth), BF16),
            vmem((1, rows), jnp.int32),
            vmem((hidden, rows), BF16),
            vmem((hidden, rows), BF16),
            vmem(flat, F32),
            vmem(flat, F32),
            vmem(blocked, BF16),
            vmem(blocked, BF16),
            vmem(blocked, BF16),
            vmem(blocked, BF16),
            vmem((rows, depth), BF16),
            vmem(grads, BF16),
            vmem(grads, BF16),
            vmem((8, 128), F32),
            vmem((8, 128), F32),
            vmem((8, 128), F32),
            vmem((8, 128), F32),
            vmem((hidden, depth), BF16),
            vmem((rows, depth), BF16),
            vmem((two * hidden, rows // GROUPS), BF16),
            dma((9,)),
            dma((2,)),
            dma((2,)),
            dma((2,)),
            dma((CHUNKS,)),
            dma((CHUNKS,)),
            dma((2, BLOCKS)),
            dma((2, BLOCKS)),
            dma((2, CHUNKS)),
            dma((2, GROUPS)),
            dma((2, 2)),
            dma((2, 3)),
            dma((CHUNKS + 1,)),
        ],
        compiler_params=pltpu.CompilerParams(
            collective_id=0, has_side_effects=True, vmem_limit_bytes=60 * 1024 * 1024
        ),
    )(
        w_pair.reshape(flat),
        w_down[0],
        tokens[0],
        cotangent[0],
        msg_left.reshape(flat),
        msg_right.reshape(flat),
        seq_ids,
        count_left,
        count_right,
    )
    return out.reshape(w_pair.shape)


def solution(mesh):
    return jax.shard_map(
        functools.partial(body, mesh.shape["chain"]),
        mesh=mesh,
        in_specs=(
            P("chain", None, "shard", None),
            P("chain", "shard", None),
            P("chain", "shard", None),
            P("chain", "shard", None),
            P("chain", "shard"),
            P("chain", None, "shard", None),
            P("chain", None, "shard", None),
            P("chain"),
            P("chain"),
        ),
        out_specs=P("chain", None, "shard", None),
        check_vma=False,
    )
```

```python
import functools

import jax
import jax.numpy as jnp
from jax import lax
from jax.experimental import pallas as pl
from jax.experimental.pallas import tpu as pltpu
from jax.sharding import PartitionSpec as P

SEQS = 8
learn_rate = 1.0

MESH = pl.DeviceIdType.MESH
F32 = jnp.float32
BF16 = jnp.bfloat16

BLOCKS = 8
CHUNKS = 8
GROUPS = 4
PER = CHUNKS // GROUPS
FIRST_PLAN = (0, 1, 1, 1, 5)
LATE_PLAN = (7, 0, 0, 0, 1)
AHEAD = 2


def reach(plan):
    total, out = 0, []
    for count in plan:
        total += count
        out.append(total)
    return out


FIRST_REACH, LATE_REACH = reach(FIRST_PLAN), reach(LATE_PLAN)


def stage_of(ends, j):
    return next(i for i, end in enumerate(ends) if j < end)


def dot_last(a, b):
    return lax.dot_general(a, b, (((1,), (1,)), ((), ())), preferred_element_type=F32)


def dot_plain(a, b):
    return lax.dot_general(a, b, (((1,), (0,)), ((), ())), preferred_element_type=F32)


def kernel(
    n,
    w_hbm, wd_hbm, tok_hbm, cot_hbm, ml_hbm, mr_hbm, ids_hbm, cl_hbm, cr_hbm,
    out_v,
    w_v, wd_v, tok_v, cot_v, mm_v, mx_v, ids_v, cl_s, cr_s,
    wdp_v, tokp_v, ids_p, gh_s, gh_r,
    acc, s_m, s_x, r_m, r_x, tf, g_s, g_x, c_m, c_x, k_m, k_x,
    g_keep,
    load_sem, ids_sem, wd_sem, gh_sem, tok_ss, tok_rs,
    msgm_sem, msgx_sem, fwd_sem, g_sem, cnt_sem, go_sem,
):
    c = lax.axis_index("chain")
    s = lax.axis_index("shard")
    odd = lax.rem(c, 2) == 1
    even = lax.rem(c, 2) == 0
    sign = 2 * lax.rem(c, 2) - 1
    mate_c, cross_c = c - sign, c + sign
    has_cross = jnp.logical_and(cross_c >= 0, cross_c < n)
    mate, cross, peer = (mate_c, s), (cross_c, s), (c, 1 - s)
    tokens, depth = tok_v.shape
    hidden = wd_v.shape[0]
    block = depth // BLOCKS
    chunk = tokens // CHUNKS
    group = tokens // GROUPS
    width_scale = depth ** (-0.5)
    batch_scale = learn_rate * (2 * tokens) ** (-0.5)

    def local(src, dst, i):
        return pltpu.make_async_copy(src, dst, load_sem.at[i])

    loads = [
        local(src, dst, i)
        for i, (src, dst) in enumerate(
            [(ids_hbm, ids_v), (tok_hbm, tok_v), (w_hbm, w_v), (wd_hbm, wd_v), (cot_hbm, cot_v)]
        )
    ]
    count_loads = [local(cl_hbm, cl_s, 7), local(cr_hbm, cr_s, 8)]
    for load in loads + count_loads:
        load.start()

    barrier = pltpu.get_barrier_semaphore()
    for where in (peer, mate):
        pl.semaphore_signal(barrier, inc=1, device_id=where, device_id_type=MESH)

    @pl.when(has_cross)
    def _():
        pl.semaphore_signal(barrier, inc=1, device_id=cross, device_id_type=MESH)

    msg_even = [local(ml_hbm, mm_v, 5), local(mr_hbm, mx_v, 6)]
    msg_odd = [local(mr_hbm, mm_v, 5), local(ml_hbm, mx_v, 6)]

    @pl.when(even)
    def _():
        for load in msg_even:
            load.start()

    @pl.when(odd)
    def _():
        for load in msg_odd:
            load.start()

    def remote(src, dst, send_sem, recv_sem, where):
        return pltpu.make_async_remote_copy(
            src_ref=src, dst_ref=dst, send_sem=send_sem, recv_sem=recv_sem, device_id=where, device_id_type=MESH
        )

    def cols(j):
        return slice(j * block, (j + 1) * block)

    def rows(k):
        return slice(k * chunk, (k + 1) * chunk)

    def span(q):
        return slice(q * group, (q + 1) * group)

    ids_copy = remote(ids_v, ids_p, ids_sem.at[0], ids_sem.at[1], peer)
    wd_early = remote(wd_hbm, wdp_v, wd_sem.at[0], wd_sem.at[1], peer)
    wd_copy = remote(wd_v, wdp_v, wd_sem.at[0], wd_sem.at[1], peer)
    gh_copy = remote(gh_s, gh_r, gh_sem.at[0], gh_sem.at[1], peer)
    tok_copy = [
        remote(tok_v.at[rows(k)], tokp_v.at[rows(k)], tok_ss.at[k], tok_rs.at[k], peer) for k in range(CHUNKS)
    ]
    msgm_copy = [remote(s_m.at[j], r_m.at[j], msgm_sem.at[0, j], msgm_sem.at[1, j], mate) for j in range(BLOCKS)]
    msgx_copy = [remote(s_x.at[j], r_x.at[j], msgx_sem.at[0, j], msgx_sem.at[1, j], cross) for j in range(BLOCKS)]

    def fwd_copy(ends, k):
        wide = ends[k // PER] * block
        return remote(tokp_v.at[rows(k), :wide], tf.at[rows(k), :wide], fwd_sem.at[0, k], fwd_sem.at[1, k], cross)

    g_copy = [remote(g_s.at[q], g_x.at[q], g_sem.at[0, q], g_sem.at[1, q], cross) for q in range(GROUPS)]
    cnt_m = remote(c_m, k_m, cnt_sem.at[0, 0], cnt_sem.at[1, 0], mate)
    cnt_x = remote(c_x, k_x, cnt_sem.at[0, 1], cnt_sem.at[1, 1], cross)

    first_cross = jnp.logical_and(even, has_cross)
    late_cross = jnp.logical_and(odd, has_cross)
    plans = ((first_cross, FIRST_REACH), (late_cross, LATE_REACH))

    @pl.when(jnp.logical_not(has_cross))
    def _():
        for ref in (r_x, tf, g_x, k_x):
            ref[...] = jnp.zeros_like(ref)

    loads[0].wait()
    for load in count_loads:
        load.wait()
    c_m[...] = jnp.full(c_m.shape, 1 + jnp.where(odd, cr_s[0], cl_s[0]), jnp.int32).astype(F32)
    c_x[...] = jnp.full(c_x.shape, 1 + jnp.where(odd, cl_s[0], cr_s[0]), jnp.int32).astype(F32)

    with jax.named_scope("barrier"):
        pl.semaphore_wait(barrier, 2 + has_cross.astype(jnp.int32))

    ids_copy.start()

    @pl.when(even)
    def _():
        wd_early.start()

    cnt_m.start()

    @pl.when(has_cross)
    def _():
        cnt_x.start()

    def gates(pre, grad_hidden):
        gate_pre, up_pre = pre[:hidden] * width_scale, pre[hidden:] * width_scale
        sig = jax.nn.sigmoid(gate_pre)
        grad_gate = grad_hidden * up_pre * sig * (1.0 + gate_pre * (1.0 - sig))
        grad_up = grad_hidden * gate_pre * sig
        return jnp.concatenate([grad_gate, grad_up], axis=0)

    def send_cross(j):
        s_x[j] = (acc[:, cols(j)] + mx_v[:, cols(j)].astype(F32)).astype(BF16)
        msgx_copy[j].start()

    def send_stage(stage, j):
        for active, ends in plans:
            if stage_of(ends, j) == stage:

                @pl.when(active)
                def _():
                    send_cross(j)

    def pre_of(rows_v):
        return dot_last(w_v[...], rows_v)

    with jax.named_scope("load"):
        for load in loads[1:3]:
            load.wait()
    pre_own = pre_of(tok_v[...])
    for load in loads[3:]:
        load.wait()
    down_own = dot_last(wd_v[...], cot_v[...])
    one_hot = (lax.broadcasted_iota(jnp.int32, (SEQS, tokens), 0) == ids_v[...]).astype(F32)
    with jax.named_scope("ids"):
        ids_copy.wait_recv()
    other_hot = (lax.broadcasted_iota(jnp.int32, (SEQS, tokens), 0) == ids_p[...]).astype(F32)
    total = jnp.sum(one_hot + other_hot, axis=1, keepdims=True)
    seq_len = jnp.sum(one_hot * total, axis=0, keepdims=True)
    tok_weight = (2 * tokens / SEQS) / seq_len * width_scale
    g_own = gates(pre_own, down_own * tok_weight).astype(BF16)
    for load in msg_even:
        load.wait()
    for j in range(BLOCKS):
        with jax.named_scope(f"half_{j}"):
            acc[:, cols(j)] = w_v[:, cols(j)].astype(F32) - dot_plain(g_own, tok_v[:, cols(j)]) * batch_scale
            send_stage(0, j)

    @pl.when(odd)
    def _():
        with jax.named_scope("go"):
            pl.semaphore_wait(go_sem, 1)
        wd_copy.start()

    for k in range(AHEAD):
        tok_copy[k].start()
    with jax.named_scope("wd_wait"):
        wd_copy.wait_recv()
    gh_s[...] = (dot_last(wdp_v[...], cot_v[...]) * tok_weight).astype(BF16)
    gh_copy.start()

    for k in range(AHEAD, CHUNKS):
        tok_copy[k].start()
    cnt_m.wait_recv()

    @pl.when(has_cross)
    def _():
        cnt_x.wait_recv()

    inverse = 1.0 / (1.0 + k_m[0:1, 0:1] + k_x[0:1, 0:1])

    def cross_grad(q):
        return g_x[q].astype(F32).T.astype(BF16)

    def wait_cross(copies):
        @pl.when(has_cross)
        def _():
            for copy in copies:
                copy.wait_recv()

    def wait_forward(ends, q):
        wait_cross(
            [fwd_copy(ends, k) for k in range(q * PER, (q + 1) * PER) if ends[q] > 0] + ([g_copy[q]] if ends[q] > 0 else [])
        )

    def own(q):
        for k in range(q * PER, (q + 1) * PER):
            with jax.named_scope(f"tok_{k}"):
                tok_copy[k].wait_recv()
            if k == CHUNKS - 2:

                @pl.when(even)
                def _():
                    pl.semaphore_signal(go_sem, inc=1, device_id=mate, device_id_type=MESH)

            for active, ends in plans:
                if ends[q] > 0:

                    @pl.when(active)
                    def _():
                        fwd_copy(ends, k).start()

        pre = pre_of(tokp_v[span(q)])
        if q == 0:
            with jax.named_scope("gh_wait"):
                gh_copy.wait_recv()
        g_now = gates(pre, gh_r[:, span(q)].astype(F32))
        g_s[q] = g_now.T.astype(BF16)
        for active, ends in plans:
            if ends[q] > 0:

                @pl.when(active)
                def _():
                    g_copy[q].start()

        return g_now.astype(BF16)

    def part(q, j, g_now):
        return acc[:, cols(j)] - dot_plain(g_now, tokp_v[span(q), cols(j)]) * batch_scale

    def own_and_update(q):
        g_now = own(q)
        first = [j for j in range(BLOCKS) if any(stage_of(ends, j) == q + 1 for _, ends in plans)]
        for some in (first, [j for j in range(BLOCKS) if j not in first]):
            for j in some:
                acc[:, cols(j)] = part(q, j, g_now)
            for j in some:
                send_stage(q + 1, j)

    def last_order(ends):
        return sorted(range(BLOCKS), key=lambda j: stage_of(ends, j) < GROUPS)

    def send_last(ends, active, j, value):
        if stage_of(ends, j) == GROUPS:
            s_x[j] = (value + mx_v[:, cols(j)].astype(F32)).astype(BF16)

            @pl.when(active)
            def _():
                msgx_copy[j].start()

    def send_mate(j, value):
        s_m[j] = (value + mm_v[:, cols(j)].astype(F32)).astype(BF16)
        msgm_copy[j].start()

    def finish_late(g_now):
        for j in last_order(LATE_REACH):
            value = part(GROUPS - 1, j, g_now)
            acc[:, cols(j)] = value
            send_last(LATE_REACH, late_cross, j, value)
            send_mate(j, value)

    def finish_first(g_now):
        for j in last_order(FIRST_REACH):
            value = part(GROUPS - 1, j, g_now)
            acc[:, cols(j)] = value
            send_last(FIRST_REACH, first_cross, j, value)
        for j in range(BLOCKS):
            send_mate(j, acc[:, cols(j)])

    def gather_late():
        with jax.named_scope("fwd_all"):
            for q in range(GROUPS):
                wait_forward(FIRST_REACH, q)
        with jax.named_scope("msgm_all"):
            for copy in msgm_copy:
                copy.wait_recv()
        starts = [stage_of(FIRST_REACH, j) for j in range(BLOCKS)]
        early = [j for j in range(BLOCKS) if starts[j] < GROUPS]
        with jax.named_scope("msgx_early"):
            wait_cross([msgx_copy[j] for j in early])
        grads = [cross_grad(q) if FIRST_REACH[q] > 0 else None for q in range(GROUPS)]
        for j in range(BLOCKS):
            value = acc[:, cols(j)] + r_m[j].astype(F32)
            if j in early:
                grad = jnp.concatenate(grads[starts[j] :], axis=1)
                value = value + r_x[j].astype(F32) - dot_plain(grad, tf[starts[j] * group :, cols(j)]) * batch_scale
                out_v[:, cols(j)] = (value * inverse).astype(BF16)
            else:
                acc[:, cols(j)] = value
        for j in range(BLOCKS):
            if j not in early:
                with jax.named_scope(f"msgx_{j}"):
                    wait_cross([msgx_copy[j]])
                out_v[:, cols(j)] = ((acc[:, cols(j)] + r_x[j].astype(F32)) * inverse).astype(BF16)

    def gather_first():
        starts = [stage_of(LATE_REACH, j) for j in range(BLOCKS)]
        for q in range(GROUPS):
            if q == GROUPS - 1:
                with jax.named_scope("msgm_all"):
                    for copy in msgm_copy:
                        copy.wait_recv()
                for j in range(BLOCKS):
                    acc[:, cols(j)] = acc[:, cols(j)] + r_m[j].astype(F32)
            with jax.named_scope(f"fwd_{q}"):
                wait_forward(LATE_REACH, q)
                wait_cross([msgx_copy[j] for j in range(BLOCKS) if starts[j] == q])
            g_now = cross_grad(q) if LATE_REACH[q] > 0 else None
            for j in range(BLOCKS):
                if starts[j] > q:
                    continue
                value = acc[:, cols(j)] - dot_plain(g_now, tf[span(q), cols(j)]) * batch_scale
                if starts[j] == q:
                    value = value + r_x[j].astype(F32)
                if q < GROUPS - 1:
                    acc[:, cols(j)] = value
                else:
                    out_v[:, cols(j)] = (value * inverse).astype(BF16)
        for j in range(BLOCKS):
            if starts[j] == GROUPS:
                with jax.named_scope(f"msgx_{j}"):
                    wait_cross([msgx_copy[j]])
                out_v[:, cols(j)] = ((acc[:, cols(j)] + r_x[j].astype(F32)) * inverse).astype(BF16)

    own_and_update(0)
    own_and_update(1)

    own_and_update(2)
    g_last = own(GROUPS - 1)
    g_keep[...] = g_last

    @pl.when(odd)
    def _():
        finish_late(g_keep[...])
        gather_late()

    @pl.when(even)
    def _():
        finish_first(g_keep[...])
        gather_first()

    with jax.named_scope("sent"):
        for copy in [ids_copy, gh_copy, cnt_m, wd_copy] + tok_copy + msgm_copy:
            copy.wait_send()

    @pl.when(has_cross)
    def _():
        for copy in msgx_copy + [cnt_x]:
            copy.wait_send()

    for active, ends in plans:

        @pl.when(active)
        def _():
            for q in range(GROUPS):
                if ends[q] > 0:
                    g_copy[q].wait_send()
                    for k in range(q * PER, (q + 1) * PER):
                        fwd_copy(ends, k).wait_send()


def body(n, w_pair, w_down, tokens, cotangent, seq_ids, msg_left, msg_right, count_left, count_right):
    _, two, hidden, depth = w_pair.shape
    rows = tokens.shape[1]
    flat = (two * hidden, depth)
    block = depth // BLOCKS
    hbm = pl.BlockSpec(memory_space=pltpu.HBM)
    dma = pltpu.SemaphoreType.DMA
    blocked = (BLOCKS, two * hidden, block)
    grads = (GROUPS, rows // GROUPS, two * hidden)
    vmem = pltpu.VMEM
    out = pl.pallas_call(
        functools.partial(kernel, n),
        out_shape=vmem(flat, BF16),
        in_specs=[hbm] * 9,
        out_specs=pl.BlockSpec(memory_space=vmem),
        scratch_shapes=[
            vmem(flat, BF16),
            vmem((hidden, depth), BF16),
            vmem((rows, depth), BF16),
            vmem((rows, depth), BF16),
            vmem(flat, BF16),
            vmem(flat, BF16),
            vmem((1, rows), jnp.int32),
            pltpu.SMEM((1,), jnp.int32),
            pltpu.SMEM((1,), jnp.int32),
            vmem((hidden, depth), BF16),
            vmem((rows, depth), BF16),
            vmem((1, rows), jnp.int32),
            vmem((hidden, rows), BF16),
            vmem((hidden, rows), BF16),
            vmem(flat, F32),
            vmem(blocked, BF16),
            vmem(blocked, BF16),
            vmem(blocked, BF16),
            vmem(blocked, BF16),
            vmem((rows, depth), BF16),
            vmem(grads, BF16),
            vmem(grads, BF16),
            vmem((8, 128), F32),
            vmem((8, 128), F32),
            vmem((8, 128), F32),
            vmem((8, 128), F32),
            vmem((two * hidden, rows // GROUPS), BF16),
            dma((9,)),
            dma((2,)),
            dma((2,)),
            dma((2,)),
            dma((CHUNKS,)),
            dma((CHUNKS,)),
            dma((2, BLOCKS)),
            dma((2, BLOCKS)),
            dma((2, CHUNKS)),
            dma((2, GROUPS)),
            dma((2, 2)),
            pltpu.SemaphoreType.REGULAR,
        ],
        compiler_params=pltpu.CompilerParams(
            collective_id=0, has_side_effects=True, vmem_limit_bytes=60 * 1024 * 1024
        ),
    )(
        w_pair.reshape(flat),
        w_down[0],
        tokens[0],
        cotangent[0],
        msg_left.reshape(flat),
        msg_right.reshape(flat),
        seq_ids,
        count_left,
        count_right,
    )
    return out.reshape(w_pair.shape)


def solution(mesh):
    return jax.shard_map(
        functools.partial(body, mesh.shape["chain"]),
        mesh=mesh,
        in_specs=(
            P("chain", None, "shard", None),
            P("chain", "shard", None),
            P("chain", "shard", None),
            P("chain", "shard", None),
            P("chain", "shard"),
            P("chain", None, "shard", None),
            P("chain", None, "shard", None),
            P("chain"),
            P("chain"),
        ),
        out_specs=P("chain", None, "shard", None),
        check_vma=False,
    )
```

```python
import functools

import jax
import jax.numpy as jnp
from jax import lax
from jax.experimental import pallas as pl
from jax.experimental.pallas import tpu as pltpu
from jax.sharding import PartitionSpec as P

SEQS = 8
learn_rate = 1.0

MESH = pl.DeviceIdType.MESH
F32 = jnp.float32
BF16 = jnp.bfloat16

BLOCKS = 8
CHUNKS = 8
GROUPS = 4
PER = CHUNKS // GROUPS
FIRST_PLAN = (0, 2, 1, 1, 4)
LATE_PLAN = (7, 0, 0, 0, 1)
AHEAD = 2


def reach(plan):
    total, out = 0, []
    for count in plan:
        total += count
        out.append(total)
    return out


FIRST_REACH, LATE_REACH = reach(FIRST_PLAN), reach(LATE_PLAN)


def stage_of(ends, j):
    return next(i for i, end in enumerate(ends) if j < end)


def dot_last(a, b):
    return lax.dot_general(a, b, (((1,), (1,)), ((), ())), preferred_element_type=F32)


def dot_plain(a, b):
    return lax.dot_general(a, b, (((1,), (0,)), ((), ())), preferred_element_type=F32)


def kernel(
    n,
    w_hbm, wd_hbm, tok_hbm, cot_hbm, ml_hbm, mr_hbm, ids_hbm, cl_hbm, cr_hbm,
    out_v,
    w_v, wd_v, tok_v, cot_v, mm_v, mx_v, ids_v, cl_s, cr_s,
    wdp_v, tokp_v, ids_p, gh_s, gh_r,
    acc, s_m, s_x, r_m, r_x, tf, g_s, g_x, c_m, c_x, k_m, k_x,
    g_keep,
    load_sem, ids_sem, wd_sem, gh_sem, tok_ss, tok_rs,
    msgm_sem, msgx_sem, fwd_sem, g_sem, cnt_sem, go_sem,
):
    c = lax.axis_index("chain")
    s = lax.axis_index("shard")
    odd = lax.rem(c, 2) == 1
    even = lax.rem(c, 2) == 0
    sign = 2 * lax.rem(c, 2) - 1
    mate_c, cross_c = c - sign, c + sign
    has_cross = jnp.logical_and(cross_c >= 0, cross_c < n)
    mate, cross, peer = (mate_c, s), (cross_c, s), (c, 1 - s)
    tokens, depth = tok_v.shape
    hidden = wd_v.shape[0]
    block = depth // BLOCKS
    chunk = tokens // CHUNKS
    group = tokens // GROUPS
    width_scale = depth ** (-0.5)
    batch_scale = learn_rate * (2 * tokens) ** (-0.5)

    def local(src, dst, i):
        return pltpu.make_async_copy(src, dst, load_sem.at[i])

    loads = [
        local(src, dst, i)
        for i, (src, dst) in enumerate(
            [(ids_hbm, ids_v), (tok_hbm, tok_v), (w_hbm, w_v), (wd_hbm, wd_v), (cot_hbm, cot_v)]
        )
    ]
    count_loads = [local(cl_hbm, cl_s, 7), local(cr_hbm, cr_s, 8)]
    for load in loads + count_loads:
        load.start()

    barrier = pltpu.get_barrier_semaphore()
    for where in (peer, mate):
        pl.semaphore_signal(barrier, inc=1, device_id=where, device_id_type=MESH)

    @pl.when(has_cross)
    def _():
        pl.semaphore_signal(barrier, inc=1, device_id=cross, device_id_type=MESH)

    msg_even = [local(ml_hbm, mm_v, 5), local(mr_hbm, mx_v, 6)]
    msg_odd = [local(mr_hbm, mm_v, 5), local(ml_hbm, mx_v, 6)]

    @pl.when(even)
    def _():
        for load in msg_even:
            load.start()

    @pl.when(odd)
    def _():
        for load in msg_odd:
            load.start()

    def remote(src, dst, send_sem, recv_sem, where):
        return pltpu.make_async_remote_copy(
            src_ref=src, dst_ref=dst, send_sem=send_sem, recv_sem=recv_sem, device_id=where, device_id_type=MESH
        )

    def cols(j):
        return slice(j * block, (j + 1) * block)

    def rows(k):
        return slice(k * chunk, (k + 1) * chunk)

    def span(q):
        return slice(q * group, (q + 1) * group)

    ids_copy = remote(ids_v, ids_p, ids_sem.at[0], ids_sem.at[1], peer)
    wd_early = remote(wd_hbm, wdp_v, wd_sem.at[0], wd_sem.at[1], peer)
    wd_copy = remote(wd_v, wdp_v, wd_sem.at[0], wd_sem.at[1], peer)
    gh_copy = remote(gh_s, gh_r, gh_sem.at[0], gh_sem.at[1], peer)
    tok_copy = [
        remote(tok_v.at[rows(k)], tokp_v.at[rows(k)], tok_ss.at[k], tok_rs.at[k], peer) for k in range(CHUNKS)
    ]
    msgm_copy = [remote(s_m.at[j], r_m.at[j], msgm_sem.at[0, j], msgm_sem.at[1, j], mate) for j in range(BLOCKS)]
    msgx_copy = [remote(s_x.at[j], r_x.at[j], msgx_sem.at[0, j], msgx_sem.at[1, j], cross) for j in range(BLOCKS)]

    def fwd_copy(ends, k):
        wide = ends[k // PER] * block
        return remote(tokp_v.at[rows(k), :wide], tf.at[rows(k), :wide], fwd_sem.at[0, k], fwd_sem.at[1, k], cross)

    g_copy = [remote(g_s.at[q], g_x.at[q], g_sem.at[0, q], g_sem.at[1, q], cross) for q in range(GROUPS)]
    cnt_m = remote(c_m, k_m, cnt_sem.at[0, 0], cnt_sem.at[1, 0], mate)
    cnt_x = remote(c_x, k_x, cnt_sem.at[0, 1], cnt_sem.at[1, 1], cross)

    first_cross = jnp.logical_and(even, has_cross)
    late_cross = jnp.logical_and(odd, has_cross)
    plans = ((first_cross, FIRST_REACH), (late_cross, LATE_REACH))

    @pl.when(jnp.logical_not(has_cross))
    def _():
        for ref in (r_x, tf, g_x, k_x):
            ref[...] = jnp.zeros_like(ref)

    loads[0].wait()
    for load in count_loads:
        load.wait()
    c_m[...] = jnp.full(c_m.shape, 1 + jnp.where(odd, cr_s[0], cl_s[0]), jnp.int32).astype(F32)
    c_x[...] = jnp.full(c_x.shape, 1 + jnp.where(odd, cl_s[0], cr_s[0]), jnp.int32).astype(F32)

    with jax.named_scope("barrier"):
        pl.semaphore_wait(barrier, 2 + has_cross.astype(jnp.int32))

    ids_copy.start()

    @pl.when(even)
    def _():
        wd_early.start()

    cnt_m.start()

    @pl.when(has_cross)
    def _():
        cnt_x.start()

    def gates(pre, grad_hidden):
        gate_pre, up_pre = pre[:hidden] * width_scale, pre[hidden:] * width_scale
        sig = jax.nn.sigmoid(gate_pre)
        grad_gate = grad_hidden * up_pre * sig * (1.0 + gate_pre * (1.0 - sig))
        grad_up = grad_hidden * gate_pre * sig
        return jnp.concatenate([grad_gate, grad_up], axis=0)

    def send_cross(j):
        s_x[j] = (acc[:, cols(j)] + mx_v[:, cols(j)].astype(F32)).astype(BF16)
        msgx_copy[j].start()

    def send_stage(stage, j):
        for active, ends in plans:
            if stage_of(ends, j) == stage:

                @pl.when(active)
                def _():
                    send_cross(j)

    def pre_of(rows_v):
        return dot_last(w_v[...], rows_v)

    with jax.named_scope("load"):
        for load in loads[1:3]:
            load.wait()
    pre_own = pre_of(tok_v[...])
    for load in loads[3:]:
        load.wait()
    down_own = dot_last(wd_v[...], cot_v[...])
    one_hot = (lax.broadcasted_iota(jnp.int32, (SEQS, tokens), 0) == ids_v[...]).astype(F32)
    with jax.named_scope("ids"):
        ids_copy.wait_recv()
    other_hot = (lax.broadcasted_iota(jnp.int32, (SEQS, tokens), 0) == ids_p[...]).astype(F32)
    total = jnp.sum(one_hot + other_hot, axis=1, keepdims=True)
    seq_len = jnp.sum(one_hot * total, axis=0, keepdims=True)
    tok_weight = (2 * tokens / SEQS) / seq_len * width_scale
    g_own = gates(pre_own, down_own * tok_weight).astype(BF16)
    for load in msg_even:
        load.wait()
    for j in range(BLOCKS):
        with jax.named_scope(f"half_{j}"):
            acc[:, cols(j)] = w_v[:, cols(j)].astype(F32) - dot_plain(g_own, tok_v[:, cols(j)]) * batch_scale
            send_stage(0, j)

    @pl.when(odd)
    def _():
        with jax.named_scope("go"):
            pl.semaphore_wait(go_sem, 1)
        wd_copy.start()

    for k in range(AHEAD):
        tok_copy[k].start()
    with jax.named_scope("wd_wait"):
        wd_copy.wait_recv()
    gh_s[...] = (dot_last(wdp_v[...], cot_v[...]) * tok_weight).astype(BF16)
    gh_copy.start()

    for k in range(AHEAD, CHUNKS):
        tok_copy[k].start()
    cnt_m.wait_recv()

    @pl.when(has_cross)
    def _():
        cnt_x.wait_recv()

    inverse = 1.0 / (1.0 + k_m[0:1, 0:1] + k_x[0:1, 0:1])

    def cross_grad(q):
        return g_x[q].astype(F32).T.astype(BF16)

    def wait_cross(copies):
        @pl.when(has_cross)
        def _():
            for copy in copies:
                copy.wait_recv()

    def wait_forward(ends, q):
        wait_cross(
            [fwd_copy(ends, k) for k in range(q * PER, (q + 1) * PER) if ends[q] > 0] + ([g_copy[q]] if ends[q] > 0 else [])
        )

    def own(q):
        for k in range(q * PER, (q + 1) * PER):
            with jax.named_scope(f"tok_{k}"):
                tok_copy[k].wait_recv()
            if k == CHUNKS - 2:

                @pl.when(even)
                def _():
                    pl.semaphore_signal(go_sem, inc=1, device_id=mate, device_id_type=MESH)

            for active, ends in plans:
                if ends[q] > 0:

                    @pl.when(active)
                    def _():
                        fwd_copy(ends, k).start()

        pre = pre_of(tokp_v[span(q)])
        if q == 0:
            with jax.named_scope("gh_wait"):
                gh_copy.wait_recv()
        g_now = gates(pre, gh_r[:, span(q)].astype(F32))
        g_s[q] = g_now.T.astype(BF16)
        for active, ends in plans:
            if ends[q] > 0:

                @pl.when(active)
                def _():
                    g_copy[q].start()

        return g_now.astype(BF16)

    def part(q, j, g_now):
        return acc[:, cols(j)] - dot_plain(g_now, tokp_v[span(q), cols(j)]) * batch_scale

    def own_and_update(q):
        g_now = own(q)
        first = [j for j in range(BLOCKS) if any(stage_of(ends, j) == q + 1 for _, ends in plans)]
        for some in (first, [j for j in range(BLOCKS) if j not in first]):
            for j in some:
                acc[:, cols(j)] = part(q, j, g_now)
            for j in some:
                send_stage(q + 1, j)

    def last_order(ends):
        return sorted(range(BLOCKS), key=lambda j: stage_of(ends, j) < GROUPS)

    def send_last(ends, active, j, value):
        if stage_of(ends, j) == GROUPS:
            s_x[j] = (value + mx_v[:, cols(j)].astype(F32)).astype(BF16)

            @pl.when(active)
            def _():
                msgx_copy[j].start()

    def send_mate(j, value):
        s_m[j] = (value + mm_v[:, cols(j)].astype(F32)).astype(BF16)
        msgm_copy[j].start()

    def finish_late(g_now):
        for j in last_order(LATE_REACH):
            value = part(GROUPS - 1, j, g_now)
            acc[:, cols(j)] = value
            send_last(LATE_REACH, late_cross, j, value)
            send_mate(j, value)

    def finish_first(g_now):
        for j in last_order(FIRST_REACH):
            value = part(GROUPS - 1, j, g_now)
            acc[:, cols(j)] = value
            send_last(FIRST_REACH, first_cross, j, value)
        for j in range(BLOCKS):
            send_mate(j, acc[:, cols(j)])

    def gather_late():
        with jax.named_scope("fwd_all"):
            for q in range(GROUPS):
                wait_forward(FIRST_REACH, q)
        with jax.named_scope("msgm_all"):
            for copy in msgm_copy:
                copy.wait_recv()
        starts = [stage_of(FIRST_REACH, j) for j in range(BLOCKS)]
        early = [j for j in range(BLOCKS) if starts[j] < GROUPS]
        with jax.named_scope("msgx_early"):
            wait_cross([msgx_copy[j] for j in early])
        grads = [cross_grad(q) if FIRST_REACH[q] > 0 else None for q in range(GROUPS)]
        for j in range(BLOCKS):
            value = acc[:, cols(j)] + r_m[j].astype(F32)
            if j in early:
                grad = jnp.concatenate(grads[starts[j] :], axis=1)
                value = value + r_x[j].astype(F32) - dot_plain(grad, tf[starts[j] * group :, cols(j)]) * batch_scale
                out_v[:, cols(j)] = (value * inverse).astype(BF16)
            else:
                acc[:, cols(j)] = value
        for j in range(BLOCKS):
            if j not in early:
                with jax.named_scope(f"msgx_{j}"):
                    wait_cross([msgx_copy[j]])
                out_v[:, cols(j)] = ((acc[:, cols(j)] + r_x[j].astype(F32)) * inverse).astype(BF16)

    def gather_first():
        starts = [stage_of(LATE_REACH, j) for j in range(BLOCKS)]
        for q in range(GROUPS):
            if q == GROUPS - 1:
                with jax.named_scope("msgm_all"):
                    for copy in msgm_copy:
                        copy.wait_recv()
                for j in range(BLOCKS):
                    acc[:, cols(j)] = acc[:, cols(j)] + r_m[j].astype(F32)
            with jax.named_scope(f"fwd_{q}"):
                wait_forward(LATE_REACH, q)
                wait_cross([msgx_copy[j] for j in range(BLOCKS) if starts[j] == q])
            g_now = cross_grad(q) if LATE_REACH[q] > 0 else None
            for j in range(BLOCKS):
                if starts[j] > q:
                    continue
                value = acc[:, cols(j)] - dot_plain(g_now, tf[span(q), cols(j)]) * batch_scale
                if starts[j] == q:
                    value = value + r_x[j].astype(F32)
                if q < GROUPS - 1:
                    acc[:, cols(j)] = value
                else:
                    out_v[:, cols(j)] = (value * inverse).astype(BF16)
        for j in range(BLOCKS):
            if starts[j] == GROUPS:
                with jax.named_scope(f"msgx_{j}"):
                    wait_cross([msgx_copy[j]])
                out_v[:, cols(j)] = ((acc[:, cols(j)] + r_x[j].astype(F32)) * inverse).astype(BF16)

    own_and_update(0)
    own_and_update(1)

    own_and_update(2)
    g_last = own(GROUPS - 1)
    g_keep[...] = g_last

    @pl.when(odd)
    def _():
        finish_late(g_keep[...])
        gather_late()

    @pl.when(even)
    def _():
        finish_first(g_keep[...])
        gather_first()

    with jax.named_scope("sent"):
        for copy in [ids_copy, gh_copy, cnt_m, wd_copy] + tok_copy + msgm_copy:
            copy.wait_send()

    @pl.when(has_cross)
    def _():
        for copy in msgx_copy + [cnt_x]:
            copy.wait_send()

    for active, ends in plans:

        @pl.when(active)
        def _():
            for q in range(GROUPS):
                if ends[q] > 0:
                    g_copy[q].wait_send()
                    for k in range(q * PER, (q + 1) * PER):
                        fwd_copy(ends, k).wait_send()


def body(n, w_pair, w_down, tokens, cotangent, seq_ids, msg_left, msg_right, count_left, count_right):
    _, two, hidden, depth = w_pair.shape
    rows = tokens.shape[1]
    flat = (two * hidden, depth)
    block = depth // BLOCKS
    hbm = pl.BlockSpec(memory_space=pltpu.HBM)
    dma = pltpu.SemaphoreType.DMA
    blocked = (BLOCKS, two * hidden, block)
    grads = (GROUPS, rows // GROUPS, two * hidden)
    vmem = pltpu.VMEM
    out = pl.pallas_call(
        functools.partial(kernel, n),
        out_shape=vmem(flat, BF16),
        in_specs=[hbm] * 9,
        out_specs=pl.BlockSpec(memory_space=vmem),
        scratch_shapes=[
            vmem(flat, BF16),
            vmem((hidden, depth), BF16),
            vmem((rows, depth), BF16),
            vmem((rows, depth), BF16),
            vmem(flat, BF16),
            vmem(flat, BF16),
            vmem((1, rows), jnp.int32),
            pltpu.SMEM((1,), jnp.int32),
            pltpu.SMEM((1,), jnp.int32),
            vmem((hidden, depth), BF16),
            vmem((rows, depth), BF16),
            vmem((1, rows), jnp.int32),
            vmem((hidden, rows), BF16),
            vmem((hidden, rows), BF16),
            vmem(flat, F32),
            vmem(blocked, BF16),
            vmem(blocked, BF16),
            vmem(blocked, BF16),
            vmem(blocked, BF16),
            vmem((rows, depth), BF16),
            vmem(grads, BF16),
            vmem(grads, BF16),
            vmem((8, 128), F32),
            vmem((8, 128), F32),
            vmem((8, 128), F32),
            vmem((8, 128), F32),
            vmem((two * hidden, rows // GROUPS), BF16),
            dma((9,)),
            dma((2,)),
            dma((2,)),
            dma((2,)),
            dma((CHUNKS,)),
            dma((CHUNKS,)),
            dma((2, BLOCKS)),
            dma((2, BLOCKS)),
            dma((2, CHUNKS)),
            dma((2, GROUPS)),
            dma((2, 2)),
            pltpu.SemaphoreType.REGULAR,
        ],
        compiler_params=pltpu.CompilerParams(
            collective_id=0, has_side_effects=True, vmem_limit_bytes=60 * 1024 * 1024
        ),
    )(
        w_pair.reshape(flat),
        w_down[0],
        tokens[0],
        cotangent[0],
        msg_left.reshape(flat),
        msg_right.reshape(flat),
        seq_ids,
        count_left,
        count_right,
    )
    return out.reshape(w_pair.shape)


def solution(mesh):
    return jax.shard_map(
        functools.partial(body, mesh.shape["chain"]),
        mesh=mesh,
        in_specs=(
            P("chain", None, "shard", None),
            P("chain", "shard", None),
            P("chain", "shard", None),
            P("chain", "shard", None),
            P("chain", "shard"),
            P("chain", None, "shard", None),
            P("chain", None, "shard", None),
            P("chain"),
            P("chain"),
        ),
        out_specs=P("chain", None, "shard", None),
        check_vma=False,
    )
```

```python
import functools

import jax
import jax.numpy as jnp
from jax import lax
from jax.experimental import pallas as pl
from jax.experimental.pallas import tpu as pltpu
from jax.sharding import PartitionSpec as P

SEQS = 8
learn_rate = 1.0

MESH = pl.DeviceIdType.MESH
F32 = jnp.float32
BF16 = jnp.bfloat16

BLOCKS = 8
CHUNKS = 8
GROUPS = 4
PER = CHUNKS // GROUPS
FIRST_PLAN = (0, 2, 1, 1, 4)
LATE_PLAN = (7, 0, 0, 0, 1)
AHEAD = 2


def reach(plan):
    total, out = 0, []
    for count in plan:
        total += count
        out.append(total)
    return out


FIRST_REACH, LATE_REACH = reach(FIRST_PLAN), reach(LATE_PLAN)


def stage_of(ends, j):
    return next(i for i, end in enumerate(ends) if j < end)


def dot_last(a, b):
    return lax.dot_general(a, b, (((1,), (1,)), ((), ())), preferred_element_type=F32)


def dot_plain(a, b):
    return lax.dot_general(a, b, (((1,), (0,)), ((), ())), preferred_element_type=F32)


def kernel(
    n,
    w_hbm, wd_hbm, tok_hbm, cot_hbm, ml_hbm, mr_hbm, ids_hbm, cl_hbm, cr_hbm,
    out_v,
    w_v, wd_v, tok_v, cot_v, mm_v, mx_v, ids_v, cl_s, cr_s,
    wdp_v, tokp_v, ids_p, gh_s, gh_r,
    acc, s_m, s_x, r_m, r_x, tf, g_s, g_x, c_m, c_x, k_m, k_x,
    g_keep,
    load_sem, ids_sem, wd_sem, gh_sem, tok_ss, tok_rs,
    msgm_sem, msgx_ss, msgx_rs, fwd_sem, g_sem, cnt_sem, go_sem,
):
    c = lax.axis_index("chain")
    s = lax.axis_index("shard")
    odd = lax.rem(c, 2) == 1
    even = lax.rem(c, 2) == 0
    sign = 2 * lax.rem(c, 2) - 1
    mate_c, cross_c = c - sign, c + sign
    has_cross = jnp.logical_and(cross_c >= 0, cross_c < n)
    mate, cross, peer = (mate_c, s), (cross_c, s), (c, 1 - s)
    tokens, depth = tok_v.shape
    hidden = wd_v.shape[0]
    block = depth // BLOCKS
    chunk = tokens // CHUNKS
    group = tokens // GROUPS
    width_scale = depth ** (-0.5)
    batch_scale = learn_rate * (2 * tokens) ** (-0.5)

    def local(src, dst, i):
        return pltpu.make_async_copy(src, dst, load_sem.at[i])

    loads = [
        local(src, dst, i)
        for i, (src, dst) in enumerate(
            [(ids_hbm, ids_v), (tok_hbm, tok_v), (w_hbm, w_v), (wd_hbm, wd_v), (cot_hbm, cot_v)]
        )
    ]
    count_loads = [local(cl_hbm, cl_s, 7), local(cr_hbm, cr_s, 8)]
    for load in loads + count_loads:
        load.start()

    barrier = pltpu.get_barrier_semaphore()
    for where in (peer, mate):
        pl.semaphore_signal(barrier, inc=1, device_id=where, device_id_type=MESH)

    @pl.when(has_cross)
    def _():
        pl.semaphore_signal(barrier, inc=1, device_id=cross, device_id_type=MESH)

    msg_even = [local(ml_hbm, mm_v, 5), local(mr_hbm, mx_v, 6)]
    msg_odd = [local(mr_hbm, mm_v, 5), local(ml_hbm, mx_v, 6)]

    @pl.when(even)
    def _():
        for load in msg_even:
            load.start()

    @pl.when(odd)
    def _():
        for load in msg_odd:
            load.start()

    def remote(src, dst, send_sem, recv_sem, where):
        return pltpu.make_async_remote_copy(
            src_ref=src, dst_ref=dst, send_sem=send_sem, recv_sem=recv_sem, device_id=where, device_id_type=MESH
        )

    def cols(j):
        return slice(j * block, (j + 1) * block)

    def rows(k):
        return slice(k * chunk, (k + 1) * chunk)

    def span(q):
        return slice(q * group, (q + 1) * group)

    ids_copy = remote(ids_v, ids_p, ids_sem.at[0], ids_sem.at[1], peer)
    wd_early = remote(wd_hbm, wdp_v, wd_sem.at[0], wd_sem.at[1], peer)
    wd_copy = remote(wd_v, wdp_v, wd_sem.at[0], wd_sem.at[1], peer)
    gh_copy = remote(gh_s, gh_r, gh_sem.at[0], gh_sem.at[1], peer)
    tok_copy = [
        remote(tok_v.at[rows(k)], tokp_v.at[rows(k)], tok_ss, tok_rs.at[k], peer) for k in range(CHUNKS)
    ]
    tok_all = remote(tok_v, tokp_v, tok_ss, tok_rs.at[0], peer)
    msgm_copy = [remote(s_m.at[j], r_m.at[j], msgm_sem.at[0], msgm_sem.at[1], mate) for j in range(BLOCKS)]
    msgm_all = remote(s_m, r_m, msgm_sem.at[0], msgm_sem.at[1], mate)

    def msgx_copy(ends, j):
        slot = max(0, j + 1 - ends[GROUPS - 1])
        return remote(s_x.at[j], r_x.at[j], msgx_ss, msgx_rs.at[slot], cross)

    def msgx_early(ends):
        early = ends[GROUPS - 1]
        return remote(s_x.at[:early], r_x.at[:early], msgx_ss, msgx_rs.at[0], cross)

    msgx_all = remote(s_x, r_x, msgx_ss, msgx_rs.at[0], cross)

    def fwd_rows(ends, q, taken):
        wide = ends[q] * block
        return remote(tokp_v.at[taken, :wide], tf.at[taken, :wide], fwd_sem.at[0, q], fwd_sem.at[1, q], cross)

    def fwd_copy(ends, k):
        return fwd_rows(ends, k // PER, rows(k))

    def fwd_group(ends, q):
        return fwd_rows(ends, q, span(q))

    g_copy = [remote(g_s.at[q], g_x.at[q], g_sem.at[0, q], g_sem.at[1, q], cross) for q in range(GROUPS)]
    cnt_m = remote(c_m, k_m, cnt_sem.at[0, 0], cnt_sem.at[1, 0], mate)
    cnt_x = remote(c_x, k_x, cnt_sem.at[0, 1], cnt_sem.at[1, 1], cross)

    first_cross = jnp.logical_and(even, has_cross)
    late_cross = jnp.logical_and(odd, has_cross)
    plans = ((first_cross, FIRST_REACH), (late_cross, LATE_REACH))

    @pl.when(jnp.logical_not(has_cross))
    def _():
        k_x[...] = jnp.zeros_like(k_x)

    loads[0].wait()
    for load in count_loads:
        load.wait()
    c_m[...] = jnp.full(c_m.shape, 1 + jnp.where(odd, cr_s[0], cl_s[0]), jnp.int32).astype(F32)
    c_x[...] = jnp.full(c_x.shape, 1 + jnp.where(odd, cl_s[0], cr_s[0]), jnp.int32).astype(F32)

    with jax.named_scope("barrier"):
        pl.semaphore_wait(barrier, 2 + has_cross.astype(jnp.int32))

    ids_copy.start()

    @pl.when(even)
    def _():
        wd_early.start()

    cnt_m.start()

    @pl.when(has_cross)
    def _():
        cnt_x.start()

    def gates(pre, grad_hidden):
        gate_pre, up_pre = pre[:hidden] * width_scale, pre[hidden:] * width_scale
        sig = jax.nn.sigmoid(gate_pre)
        grad_gate = grad_hidden * up_pre * sig * (1.0 + gate_pre * (1.0 - sig))
        grad_up = grad_hidden * gate_pre * sig
        return jnp.concatenate([grad_gate, grad_up], axis=0)

    def send_cross(ends, j):
        s_x[j] = (acc[:, cols(j)] + mx_v[:, cols(j)].astype(F32)).astype(BF16)
        msgx_copy(ends, j).start()

    def send_stage(stage, j):
        for active, ends in plans:
            if stage_of(ends, j) == stage:

                @pl.when(active)
                def _():
                    send_cross(ends, j)

    def pre_of(rows_v):
        return dot_last(w_v[...], rows_v)

    with jax.named_scope("load"):
        for load in loads[1:3]:
            load.wait()
    pre_own = pre_of(tok_v[...])
    for load in loads[3:]:
        load.wait()
    down_own = dot_last(wd_v[...], cot_v[...])
    one_hot = (lax.broadcasted_iota(jnp.int32, (SEQS, tokens), 0) == ids_v[...]).astype(F32)
    with jax.named_scope("ids"):
        ids_copy.wait_recv()
    other_hot = (lax.broadcasted_iota(jnp.int32, (SEQS, tokens), 0) == ids_p[...]).astype(F32)
    total = jnp.sum(one_hot + other_hot, axis=1, keepdims=True)
    seq_len = jnp.sum(one_hot * total, axis=0, keepdims=True)
    tok_weight = (2 * tokens / SEQS) / seq_len * width_scale
    g_own = gates(pre_own, down_own * tok_weight).astype(BF16)
    for load in msg_even:
        load.wait()
    for j in range(BLOCKS):
        with jax.named_scope(f"half_{j}"):
            acc[:, cols(j)] = w_v[:, cols(j)].astype(F32) - dot_plain(g_own, tok_v[:, cols(j)]) * batch_scale
            send_stage(0, j)

    @pl.when(odd)
    def _():
        with jax.named_scope("go"):
            pl.semaphore_wait(go_sem, 1)
        wd_copy.start()

    for k in range(AHEAD):
        tok_copy[k].start()
    with jax.named_scope("wd_wait"):
        wd_copy.wait_recv()
    gh_s[...] = (dot_last(wdp_v[...], cot_v[...]) * tok_weight).astype(BF16)
    gh_copy.start()

    for k in range(AHEAD, CHUNKS):
        tok_copy[k].start()
    cnt_m.wait_recv()

    @pl.when(has_cross)
    def _():
        cnt_x.wait_recv()

    inverse = 1.0 / (1.0 + k_m[0:1, 0:1] + k_x[0:1, 0:1])

    def cross_grad(q):
        return g_x[q].astype(F32).T.astype(BF16)

    def wait_forward(ends, q):
        if ends[q] > 0:
            fwd_group(ends, q).wait_recv()
            g_copy[q].wait_recv()

    def own(q):
        for k in range(q * PER, (q + 1) * PER):
            with jax.named_scope(f"tok_{k}"):
                tok_copy[k].wait_recv()
            if k == CHUNKS - 2:

                @pl.when(even)
                def _():
                    pl.semaphore_signal(go_sem, inc=1, device_id=mate, device_id_type=MESH)

            for active, ends in plans:
                if ends[q] > 0:

                    @pl.when(active)
                    def _():
                        fwd_copy(ends, k).start()

        pre = pre_of(tokp_v[span(q)])
        if q == 0:
            with jax.named_scope("gh_wait"):
                gh_copy.wait_recv()
        g_now = gates(pre, gh_r[:, span(q)].astype(F32))
        g_s[q] = g_now.T.astype(BF16)
        for active, ends in plans:
            if ends[q] > 0:

                @pl.when(active)
                def _():
                    g_copy[q].start()

        return g_now.astype(BF16)

    def part(q, j, g_now):
        return acc[:, cols(j)] - dot_plain(g_now, tokp_v[span(q), cols(j)]) * batch_scale

    def own_and_update(q):
        g_now = own(q)
        first = [j for j in range(BLOCKS) if any(stage_of(ends, j) == q + 1 for _, ends in plans)]
        for some in (first, [j for j in range(BLOCKS) if j not in first]):
            for j in some:
                acc[:, cols(j)] = part(q, j, g_now)
            for j in some:
                send_stage(q + 1, j)

    def last_order(ends):
        return sorted(range(BLOCKS), key=lambda j: stage_of(ends, j) < GROUPS)

    def send_last(ends, active, j, value):
        if stage_of(ends, j) == GROUPS:
            s_x[j] = (value + mx_v[:, cols(j)].astype(F32)).astype(BF16)

            @pl.when(active)
            def _():
                msgx_copy(ends, j).start()

    def send_mate(j, value):
        s_m[j] = (value + mm_v[:, cols(j)].astype(F32)).astype(BF16)
        msgm_copy[j].start()

    def finish_late(g_now):
        for j in last_order(LATE_REACH):
            value = part(GROUPS - 1, j, g_now)
            acc[:, cols(j)] = value
            send_last(LATE_REACH, late_cross, j, value)
            send_mate(j, value)

    def finish_first(g_now):
        for j in last_order(FIRST_REACH):
            value = part(GROUPS - 1, j, g_now)
            acc[:, cols(j)] = value
            send_last(FIRST_REACH, first_cross, j, value)
        for j in range(BLOCKS):
            send_mate(j, acc[:, cols(j)])

    def gather_late():
        with jax.named_scope("fwd_all"):
            for q in range(GROUPS):
                wait_forward(FIRST_REACH, q)
        with jax.named_scope("msgm_all"):
            msgm_all.wait_recv()
        starts = [stage_of(FIRST_REACH, j) for j in range(BLOCKS)]
        early = [j for j in range(BLOCKS) if starts[j] < GROUPS]
        with jax.named_scope("msgx_early"):
            if early:
                msgx_early(FIRST_REACH).wait_recv()
        grads = [cross_grad(q) if FIRST_REACH[q] > 0 else None for q in range(GROUPS)]
        for j in range(BLOCKS):
            value = acc[:, cols(j)] + r_m[j].astype(F32)
            if j in early:
                grad = jnp.concatenate(grads[starts[j] :], axis=1)
                value = value + r_x[j].astype(F32) - dot_plain(grad, tf[starts[j] * group :, cols(j)]) * batch_scale
                out_v[:, cols(j)] = (value * inverse).astype(BF16)
            else:
                acc[:, cols(j)] = value
        for j in range(BLOCKS):
            if j not in early:
                with jax.named_scope(f"msgx_{j}"):
                    msgx_copy(FIRST_REACH, j).wait_recv()
                out_v[:, cols(j)] = ((acc[:, cols(j)] + r_x[j].astype(F32)) * inverse).astype(BF16)

    def gather_alone():
        msgm_all.wait_recv()
        for j in range(BLOCKS):
            out_v[:, cols(j)] = ((acc[:, cols(j)] + r_m[j].astype(F32)) * inverse).astype(BF16)

    def gather_first():
        starts = [stage_of(LATE_REACH, j) for j in range(BLOCKS)]
        for q in range(GROUPS):
            if q == GROUPS - 1:
                with jax.named_scope("msgm_all"):
                    msgm_all.wait_recv()
                for j in range(BLOCKS):
                    acc[:, cols(j)] = acc[:, cols(j)] + r_m[j].astype(F32)
            with jax.named_scope(f"fwd_{q}"):
                wait_forward(LATE_REACH, q)
                if q == starts[0]:
                    msgx_early(LATE_REACH).wait_recv()
            g_now = cross_grad(q) if LATE_REACH[q] > 0 else None
            for j in range(BLOCKS):
                if starts[j] > q:
                    continue
                value = acc[:, cols(j)] - dot_plain(g_now, tf[span(q), cols(j)]) * batch_scale
                if starts[j] == q:
                    value = value + r_x[j].astype(F32)
                if q < GROUPS - 1:
                    acc[:, cols(j)] = value
                else:
                    out_v[:, cols(j)] = (value * inverse).astype(BF16)
        for j in range(BLOCKS):
            if starts[j] == GROUPS:
                with jax.named_scope(f"msgx_{j}"):
                    msgx_copy(LATE_REACH, j).wait_recv()
                out_v[:, cols(j)] = ((acc[:, cols(j)] + r_x[j].astype(F32)) * inverse).astype(BF16)

    own_and_update(0)
    own_and_update(1)

    own_and_update(2)
    g_last = own(GROUPS - 1)
    g_keep[...] = g_last

    @pl.when(odd)
    def _():
        finish_late(g_keep[...])

    @pl.when(even)
    def _():
        finish_first(g_keep[...])

    @pl.when(late_cross)
    def _():
        gather_late()

    @pl.when(first_cross)
    def _():
        gather_first()

    @pl.when(jnp.logical_not(has_cross))
    def _():
        gather_alone()

    with jax.named_scope("sent"):
        for copy in [ids_copy, gh_copy, cnt_m, wd_copy, tok_all, msgm_all]:
            copy.wait_send()

    @pl.when(has_cross)
    def _():
        for copy in (msgx_all, cnt_x):
            copy.wait_send()

    for active, ends in plans:

        @pl.when(active)
        def _():
            for q in range(GROUPS):
                if ends[q] > 0:
                    g_copy[q].wait_send()
                    fwd_group(ends, q).wait_send()


def body(n, w_pair, w_down, tokens, cotangent, seq_ids, msg_left, msg_right, count_left, count_right):
    _, two, hidden, depth = w_pair.shape
    rows = tokens.shape[1]
    flat = (two * hidden, depth)
    block = depth // BLOCKS
    hbm = pl.BlockSpec(memory_space=pltpu.HBM)
    dma = pltpu.SemaphoreType.DMA
    blocked = (BLOCKS, two * hidden, block)
    grads = (GROUPS, rows // GROUPS, two * hidden)
    vmem = pltpu.VMEM
    out = pl.pallas_call(
        functools.partial(kernel, n),
        out_shape=vmem(flat, BF16),
        in_specs=[hbm] * 9,
        out_specs=pl.BlockSpec(memory_space=vmem),
        scratch_shapes=[
            vmem(flat, BF16),
            vmem((hidden, depth), BF16),
            vmem((rows, depth), BF16),
            vmem((rows, depth), BF16),
            vmem(flat, BF16),
            vmem(flat, BF16),
            vmem((1, rows), jnp.int32),
            pltpu.SMEM((1,), jnp.int32),
            pltpu.SMEM((1,), jnp.int32),
            vmem((hidden, depth), BF16),
            vmem((rows, depth), BF16),
            vmem((1, rows), jnp.int32),
            vmem((hidden, rows), BF16),
            vmem((hidden, rows), BF16),
            vmem(flat, F32),
            vmem(blocked, BF16),
            vmem(blocked, BF16),
            vmem(blocked, BF16),
            vmem(blocked, BF16),
            vmem((rows, depth), BF16),
            vmem(grads, BF16),
            vmem(grads, BF16),
            vmem((8, 128), F32),
            vmem((8, 128), F32),
            vmem((8, 128), F32),
            vmem((8, 128), F32),
            vmem((two * hidden, rows // GROUPS), BF16),
            dma((9,)),
            dma((2,)),
            dma((2,)),
            dma((2,)),
            dma(()),
            dma((CHUNKS,)),
            dma((2,)),
            dma(()),
            dma((1 + BLOCKS - min(FIRST_REACH[GROUPS - 1], LATE_REACH[GROUPS - 1]),)),
            dma((2, GROUPS)),
            dma((2, GROUPS)),
            dma((2, 2)),
            pltpu.SemaphoreType.REGULAR,
        ],
        compiler_params=pltpu.CompilerParams(
            collective_id=0, has_side_effects=True, vmem_limit_bytes=60 * 1024 * 1024
        ),
    )(
        w_pair.reshape(flat),
        w_down[0],
        tokens[0],
        cotangent[0],
        msg_left.reshape(flat),
        msg_right.reshape(flat),
        seq_ids,
        count_left,
        count_right,
    )
    return out.reshape(w_pair.shape)


def solution(mesh):
    return jax.shard_map(
        functools.partial(body, mesh.shape["chain"]),
        mesh=mesh,
        in_specs=(
            P("chain", None, "shard", None),
            P("chain", "shard", None),
            P("chain", "shard", None),
            P("chain", "shard", None),
            P("chain", "shard"),
            P("chain", None, "shard", None),
            P("chain", None, "shard", None),
            P("chain"),
            P("chain"),
        ),
        out_specs=P("chain", None, "shard", None),
        check_vma=False,
    )
```

```python
import functools

import jax
import jax.numpy as jnp
from jax import lax
from jax.experimental import pallas as pl
from jax.experimental.pallas import tpu as pltpu
from jax.sharding import PartitionSpec as P

SEQS = 8
learn_rate = 1.0

MESH = pl.DeviceIdType.MESH
F32 = jnp.float32
BF16 = jnp.bfloat16

BLOCKS = 8
CHUNKS = 8
GROUPS = 4
PER = CHUNKS // GROUPS
FIRST_PLAN = (0, 2, 1, 1, 4)
LATE_PLAN = (7, 0, 0, 0, 1)
AHEAD = 2


def reach(plan):
    total, out = 0, []
    for count in plan:
        total += count
        out.append(total)
    return out


FIRST_REACH, LATE_REACH = reach(FIRST_PLAN), reach(LATE_PLAN)


def stage_of(ends, j):
    return next(i for i, end in enumerate(ends) if j < end)


def dot_last(a, b):
    return lax.dot_general(a, b, (((1,), (1,)), ((), ())), preferred_element_type=F32)


def dot_plain(a, b):
    return lax.dot_general(a, b, (((1,), (0,)), ((), ())), preferred_element_type=F32)


def kernel(
    n,
    w_hbm, wd_hbm, tok_hbm, cot_hbm, ml_hbm, mr_hbm, ids_hbm, cl_hbm, cr_hbm,
    out_v,
    w_v, wd_v, tok_v, cot_v, mm_v, mx_v, ids_v, cl_s, cr_s,
    wdp_v, tokp_v, ids_p, gh_s, gh_r,
    acc, s_m, s_x, r_m, r_x, tf, g_s, g_x, c_m, c_x, k_m, k_x,
    g_keep,
    load_sem, ids_sem, wd_sem, gh_sem, tok_ss, tok_rs,
    msgm_sem, msgx_ss, msgx_rs, fwd_sem, g_sem, cnt_sem, go_sem,
):
    c = lax.axis_index("chain")
    s = lax.axis_index("shard")
    odd = lax.rem(c, 2) == 1
    even = lax.rem(c, 2) == 0
    sign = 2 * lax.rem(c, 2) - 1
    mate_c, cross_c = c - sign, c + sign
    has_cross = jnp.logical_and(cross_c >= 0, cross_c < n)
    mate, cross, peer = (mate_c, s), (cross_c, s), (c, 1 - s)
    tokens, depth = tok_v.shape
    hidden = wd_v.shape[0]
    block = depth // BLOCKS
    chunk = tokens // CHUNKS
    group = tokens // GROUPS
    width_scale = depth ** (-0.5)
    batch_scale = learn_rate * (2 * tokens) ** (-0.5)

    def local(src, dst, i):
        return pltpu.make_async_copy(src, dst, load_sem.at[i])

    loads = [
        local(src, dst, i)
        for i, (src, dst) in enumerate(
            [(ids_hbm, ids_v), (tok_hbm, tok_v), (w_hbm, w_v), (wd_hbm, wd_v), (cot_hbm, cot_v)]
        )
    ]
    count_loads = [local(cl_hbm, cl_s, 7), local(cr_hbm, cr_s, 8)]
    for load in loads + count_loads:
        load.start()

    barrier = pltpu.get_barrier_semaphore()
    for where in (peer, mate):
        pl.semaphore_signal(barrier, inc=1, device_id=where, device_id_type=MESH)

    @pl.when(has_cross)
    def _():
        pl.semaphore_signal(barrier, inc=1, device_id=cross, device_id_type=MESH)

    msg_even = [local(ml_hbm, mm_v, 5), local(mr_hbm, mx_v, 6)]
    msg_odd = [local(mr_hbm, mm_v, 5), local(ml_hbm, mx_v, 6)]

    @pl.when(even)
    def _():
        for load in msg_even:
            load.start()

    @pl.when(odd)
    def _():
        for load in msg_odd:
            load.start()

    def remote(src, dst, send_sem, recv_sem, where):
        return pltpu.make_async_remote_copy(
            src_ref=src, dst_ref=dst, send_sem=send_sem, recv_sem=recv_sem, device_id=where, device_id_type=MESH
        )

    def cols(j):
        return slice(j * block, (j + 1) * block)

    def rows(k):
        return slice(k * chunk, (k + 1) * chunk)

    def span(q):
        return slice(q * group, (q + 1) * group)

    ids_copy = remote(ids_v, ids_p, ids_sem.at[0], ids_sem.at[1], peer)
    wd_early = remote(wd_hbm, wdp_v, wd_sem.at[0], wd_sem.at[1], peer)
    wd_copy = remote(wd_v, wdp_v, wd_sem.at[0], wd_sem.at[1], peer)
    gh_copy = remote(gh_s, gh_r, gh_sem.at[0], gh_sem.at[1], peer)
    tok_copy = [
        remote(tok_v.at[rows(k)], tokp_v.at[rows(k)], tok_ss, tok_rs.at[k], peer) for k in range(CHUNKS)
    ]
    tok_all = remote(tok_v, tokp_v, tok_ss, tok_rs.at[0], peer)
    msgm_copy = [remote(s_m.at[j], r_m.at[j], msgm_sem.at[0], msgm_sem.at[1], mate) for j in range(BLOCKS)]
    msgm_all = remote(s_m, r_m, msgm_sem.at[0], msgm_sem.at[1], mate)

    def msgx_copy(ends, j):
        slot = max(0, j + 1 - ends[GROUPS - 1])
        return remote(s_x.at[j], r_x.at[j], msgx_ss, msgx_rs.at[slot], cross)

    def msgx_early(ends):
        early = ends[GROUPS - 1]
        return remote(s_x.at[:early], r_x.at[:early], msgx_ss, msgx_rs.at[0], cross)

    msgx_all = remote(s_x, r_x, msgx_ss, msgx_rs.at[0], cross)

    def fwd_rows(ends, q, taken):
        wide = ends[q] * block
        return remote(tokp_v.at[taken, :wide], tf.at[taken, :wide], fwd_sem.at[0, q], fwd_sem.at[1, q], cross)

    def fwd_copy(ends, k):
        return fwd_rows(ends, k // PER, rows(k))

    def fwd_group(ends, q):
        return fwd_rows(ends, q, span(q))

    g_copy = [remote(g_s.at[q], g_x.at[q], g_sem.at[0, q], g_sem.at[1, q], cross) for q in range(GROUPS)]
    cnt_m = remote(c_m, k_m, cnt_sem.at[0, 0], cnt_sem.at[1, 0], mate)
    cnt_x = remote(c_x, k_x, cnt_sem.at[0, 1], cnt_sem.at[1, 1], cross)

    first_cross = jnp.logical_and(even, has_cross)
    late_cross = jnp.logical_and(odd, has_cross)
    plans = ((first_cross, FIRST_REACH), (late_cross, LATE_REACH))

    @pl.when(jnp.logical_not(has_cross))
    def _():
        k_x[...] = jnp.zeros_like(k_x)

    loads[0].wait()
    with jax.named_scope("barrier"):
        pl.semaphore_wait(barrier, 2 + has_cross.astype(jnp.int32))

    ids_copy.start()

    @pl.when(even)
    def _():
        wd_early.start()

    for load in count_loads:
        load.wait()
    c_m[...] = jnp.full(c_m.shape, 1 + jnp.where(odd, cr_s[0], cl_s[0]), jnp.int32).astype(F32)
    c_x[...] = jnp.full(c_x.shape, 1 + jnp.where(odd, cl_s[0], cr_s[0]), jnp.int32).astype(F32)

    cnt_m.start()

    @pl.when(has_cross)
    def _():
        cnt_x.start()

    def gates(pre, grad_hidden):
        gate_pre, up_pre = pre[:hidden] * width_scale, pre[hidden:] * width_scale
        sig = jax.nn.sigmoid(gate_pre)
        grad_gate = grad_hidden * up_pre * sig * (1.0 + gate_pre * (1.0 - sig))
        grad_up = grad_hidden * gate_pre * sig
        return jnp.concatenate([grad_gate, grad_up], axis=0)

    def send_cross(ends, j):
        s_x[j] = (acc[:, cols(j)] + mx_v[:, cols(j)].astype(F32)).astype(BF16)
        msgx_copy(ends, j).start()

    def send_stage(stage, j):
        for active, ends in plans:
            if stage_of(ends, j) == stage:

                @pl.when(active)
                def _():
                    send_cross(ends, j)

    def pre_of(rows_v):
        return dot_last(w_v[...], rows_v)

    with jax.named_scope("load"):
        for load in loads[1:3]:
            load.wait()
    pre_own = pre_of(tok_v[...])
    for load in loads[3:]:
        load.wait()
    down_own = dot_last(wd_v[...], cot_v[...])
    one_hot = (lax.broadcasted_iota(jnp.int32, (SEQS, tokens), 0) == ids_v[...]).astype(F32)
    with jax.named_scope("ids"):
        ids_copy.wait_recv()
    other_hot = (lax.broadcasted_iota(jnp.int32, (SEQS, tokens), 0) == ids_p[...]).astype(F32)
    total = jnp.sum(one_hot + other_hot, axis=1, keepdims=True)
    seq_len = jnp.sum(one_hot * total, axis=0, keepdims=True)
    tok_weight = (2 * tokens / SEQS) / seq_len * width_scale
    g_own = gates(pre_own, down_own * tok_weight).astype(BF16)
    for load in msg_even:
        load.wait()
    for j in range(BLOCKS):
        with jax.named_scope(f"half_{j}"):
            acc[:, cols(j)] = w_v[:, cols(j)].astype(F32) - dot_plain(g_own, tok_v[:, cols(j)]) * batch_scale
            send_stage(0, j)

    @pl.when(odd)
    def _():
        with jax.named_scope("go"):
            pl.semaphore_wait(go_sem, 1)
        wd_copy.start()

    for k in range(AHEAD):
        tok_copy[k].start()
    with jax.named_scope("wd_wait"):
        wd_copy.wait_recv()
    gh_s[...] = (dot_last(wdp_v[...], cot_v[...]) * tok_weight).astype(BF16)
    gh_copy.start()

    for k in range(AHEAD, CHUNKS):
        tok_copy[k].start()
    cnt_m.wait_recv()

    @pl.when(has_cross)
    def _():
        cnt_x.wait_recv()

    inverse = 1.0 / (1.0 + k_m[0:1, 0:1] + k_x[0:1, 0:1])

    def cross_grad(q):
        return g_x[q].astype(F32).T.astype(BF16)

    def wait_forward(ends, q):
        if ends[q] > 0:
            fwd_group(ends, q).wait_recv()
            g_copy[q].wait_recv()

    def own(q):
        for k in range(q * PER, (q + 1) * PER):
            with jax.named_scope(f"tok_{k}"):
                tok_copy[k].wait_recv()
            if k == CHUNKS - 2:

                @pl.when(even)
                def _():
                    pl.semaphore_signal(go_sem, inc=1, device_id=mate, device_id_type=MESH)

            for active, ends in plans:
                if ends[q] > 0:

                    @pl.when(active)
                    def _():
                        fwd_copy(ends, k).start()

        pre = pre_of(tokp_v[span(q)])
        if q == 0:
            with jax.named_scope("gh_wait"):
                gh_copy.wait_recv()
        g_now = gates(pre, gh_r[:, span(q)].astype(F32))
        g_s[q] = g_now.T.astype(BF16)
        for active, ends in plans:
            if ends[q] > 0:

                @pl.when(active)
                def _():
                    g_copy[q].start()

        return g_now.astype(BF16)

    def part(q, j, g_now):
        return acc[:, cols(j)] - dot_plain(g_now, tokp_v[span(q), cols(j)]) * batch_scale

    def own_and_update(q):
        g_now = own(q)
        first = [j for j in range(BLOCKS) if any(stage_of(ends, j) == q + 1 for _, ends in plans)]
        for some in (first, [j for j in range(BLOCKS) if j not in first]):
            for j in some:
                acc[:, cols(j)] = part(q, j, g_now)
            for j in some:
                send_stage(q + 1, j)

    def last_order(ends):
        return sorted(range(BLOCKS), key=lambda j: stage_of(ends, j) < GROUPS)

    def send_last(ends, active, j, value):
        if stage_of(ends, j) == GROUPS:
            s_x[j] = (value + mx_v[:, cols(j)].astype(F32)).astype(BF16)

            @pl.when(active)
            def _():
                msgx_copy(ends, j).start()

    def send_mate(j, value):
        s_m[j] = (value + mm_v[:, cols(j)].astype(F32)).astype(BF16)
        msgm_copy[j].start()

    def finish_late(g_now):
        for j in last_order(LATE_REACH):
            value = part(GROUPS - 1, j, g_now)
            acc[:, cols(j)] = value
            send_last(LATE_REACH, late_cross, j, value)
            send_mate(j, value)

    def finish_first(g_now):
        for j in last_order(FIRST_REACH):
            value = part(GROUPS - 1, j, g_now)
            acc[:, cols(j)] = value
            send_last(FIRST_REACH, first_cross, j, value)
        for j in range(BLOCKS):
            send_mate(j, acc[:, cols(j)])

    def gather_late():
        with jax.named_scope("fwd_all"):
            for q in range(GROUPS):
                wait_forward(FIRST_REACH, q)
        with jax.named_scope("msgm_all"):
            msgm_all.wait_recv()
        starts = [stage_of(FIRST_REACH, j) for j in range(BLOCKS)]
        early = [j for j in range(BLOCKS) if starts[j] < GROUPS]
        with jax.named_scope("msgx_early"):
            if early:
                msgx_early(FIRST_REACH).wait_recv()
        grads = [cross_grad(q) if FIRST_REACH[q] > 0 else None for q in range(GROUPS)]
        for j in range(BLOCKS):
            value = acc[:, cols(j)] + r_m[j].astype(F32)
            if j in early:
                grad = jnp.concatenate(grads[starts[j] :], axis=1)
                value = value + r_x[j].astype(F32) - dot_plain(grad, tf[starts[j] * group :, cols(j)]) * batch_scale
                out_v[:, cols(j)] = (value * inverse).astype(BF16)
            else:
                acc[:, cols(j)] = value
        for j in range(BLOCKS):
            if j not in early:
                with jax.named_scope(f"msgx_{j}"):
                    msgx_copy(FIRST_REACH, j).wait_recv()
                out_v[:, cols(j)] = ((acc[:, cols(j)] + r_x[j].astype(F32)) * inverse).astype(BF16)

    def gather_alone():
        msgm_all.wait_recv()
        for j in range(BLOCKS):
            out_v[:, cols(j)] = ((acc[:, cols(j)] + r_m[j].astype(F32)) * inverse).astype(BF16)

    def gather_first():
        starts = [stage_of(LATE_REACH, j) for j in range(BLOCKS)]
        for q in range(GROUPS):
            if q == GROUPS - 1:
                with jax.named_scope("msgm_all"):
                    msgm_all.wait_recv()
                for j in range(BLOCKS):
                    acc[:, cols(j)] = acc[:, cols(j)] + r_m[j].astype(F32)
            with jax.named_scope(f"fwd_{q}"):
                wait_forward(LATE_REACH, q)
                if q == starts[0]:
                    msgx_early(LATE_REACH).wait_recv()
            g_now = cross_grad(q) if LATE_REACH[q] > 0 else None
            for j in range(BLOCKS):
                if starts[j] > q:
                    continue
                value = acc[:, cols(j)] - dot_plain(g_now, tf[span(q), cols(j)]) * batch_scale
                if starts[j] == q:
                    value = value + r_x[j].astype(F32)
                if q < GROUPS - 1:
                    acc[:, cols(j)] = value
                else:
                    out_v[:, cols(j)] = (value * inverse).astype(BF16)
        for j in range(BLOCKS):
            if starts[j] == GROUPS:
                with jax.named_scope(f"msgx_{j}"):
                    msgx_copy(LATE_REACH, j).wait_recv()
                out_v[:, cols(j)] = ((acc[:, cols(j)] + r_x[j].astype(F32)) * inverse).astype(BF16)

    own_and_update(0)
    own_and_update(1)

    own_and_update(2)
    g_last = own(GROUPS - 1)
    g_keep[...] = g_last

    @pl.when(odd)
    def _():
        finish_late(g_keep[...])

    @pl.when(even)
    def _():
        finish_first(g_keep[...])

    @pl.when(late_cross)
    def _():
        gather_late()

    @pl.when(first_cross)
    def _():
        gather_first()

    @pl.when(jnp.logical_not(has_cross))
    def _():
        gather_alone()

    with jax.named_scope("sent"):
        for copy in [ids_copy, gh_copy, cnt_m, wd_copy, tok_all, msgm_all]:
            copy.wait_send()

    @pl.when(has_cross)
    def _():
        for copy in (msgx_all, cnt_x):
            copy.wait_send()

    for active, ends in plans:

        @pl.when(active)
        def _():
            for q in range(GROUPS):
                if ends[q] > 0:
                    g_copy[q].wait_send()
                    fwd_group(ends, q).wait_send()


def body(n, w_pair, w_down, tokens, cotangent, seq_ids, msg_left, msg_right, count_left, count_right):
    _, two, hidden, depth = w_pair.shape
    rows = tokens.shape[1]
    flat = (two * hidden, depth)
    block = depth // BLOCKS
    hbm = pl.BlockSpec(memory_space=pltpu.HBM)
    dma = pltpu.SemaphoreType.DMA
    blocked = (BLOCKS, two * hidden, block)
    grads = (GROUPS, rows // GROUPS, two * hidden)
    vmem = pltpu.VMEM
    out = pl.pallas_call(
        functools.partial(kernel, n),
        out_shape=vmem(flat, BF16),
        in_specs=[hbm] * 9,
        out_specs=pl.BlockSpec(memory_space=vmem),
        scratch_shapes=[
            vmem(flat, BF16),
            vmem((hidden, depth), BF16),
            vmem((rows, depth), BF16),
            vmem((rows, depth), BF16),
            vmem(flat, BF16),
            vmem(flat, BF16),
            vmem((1, rows), jnp.int32),
            pltpu.SMEM((1,), jnp.int32),
            pltpu.SMEM((1,), jnp.int32),
            vmem((hidden, depth), BF16),
            vmem((rows, depth), BF16),
            vmem((1, rows), jnp.int32),
            vmem((hidden, rows), BF16),
            vmem((hidden, rows), BF16),
            vmem(flat, F32),
            vmem(blocked, BF16),
            vmem(blocked, BF16),
            vmem(blocked, BF16),
            vmem(blocked, BF16),
            vmem((rows, depth), BF16),
            vmem(grads, BF16),
            vmem(grads, BF16),
            vmem((8, 128), F32),
            vmem((8, 128), F32),
            vmem((8, 128), F32),
            vmem((8, 128), F32),
            vmem((two * hidden, rows // GROUPS), BF16),
            dma((9,)),
            dma((2,)),
            dma((2,)),
            dma((2,)),
            dma(()),
            dma((CHUNKS,)),
            dma((2,)),
            dma(()),
            dma((1 + BLOCKS - min(FIRST_REACH[GROUPS - 1], LATE_REACH[GROUPS - 1]),)),
            dma((2, GROUPS)),
            dma((2, GROUPS)),
            dma((2, 2)),
            pltpu.SemaphoreType.REGULAR,
        ],
        compiler_params=pltpu.CompilerParams(
            collective_id=0, has_side_effects=True, vmem_limit_bytes=60 * 1024 * 1024
        ),
    )(
        w_pair.reshape(flat),
        w_down[0],
        tokens[0],
        cotangent[0],
        msg_left.reshape(flat),
        msg_right.reshape(flat),
        seq_ids,
        count_left,
        count_right,
    )
    return out.reshape(w_pair.shape)


def solution(mesh):
    return jax.shard_map(
        functools.partial(body, mesh.shape["chain"]),
        mesh=mesh,
        in_specs=(
            P("chain", None, "shard", None),
            P("chain", "shard", None),
            P("chain", "shard", None),
            P("chain", "shard", None),
            P("chain", "shard"),
            P("chain", None, "shard", None),
            P("chain", None, "shard", None),
            P("chain"),
            P("chain"),
        ),
        out_specs=P("chain", None, "shard", None),
        check_vma=False,
    )
```
